16 devices in a mesh: dp: 4 (over y, z, core), tp: 4 (over x).
Axes of the slice: x: 4, y: 2, z: 1, core: 2. Of those that a mesh axis runs over, the one named last changes fastest.
The devices are a block of a 4x4x8 slice.
Arguments:
- x: bfloat16 [4096, 7168], P(('dp', 'tp')), parts along dimension 0
- gain: bfloat16 [7168], replicated
- wq: bfloat16 [7168, 7168], P(None, 'tp')
- wk: bfloat16 [7168, 7168], P(None, 'tp')
- wv: bfloat16 [7168, 7168], P(None, 'tp')
- wo: bfloat16 [7168, 7168], P('tp')
Outputs:
- output: bfloat16 [4096, 7168], P(('dp', 'tp')), parts along dimension 0
There are 4 independent parts. The reference program is written for one: setup_inputs(seed, part) draws one part's arguments, and reference() takes and returns one part's arrays. A program takes and returns all parts, laid end to end along the dimension named above; an argument that names none is the same for every part.
All inputs are finite; a program needn't handle non-finite values.
Results may differ from the reference program's by a relative error of at most 0.012.
Values are sent between devices in bfloat16 or wider.
A program may use at most 768 MiB of HBM per device.

```python
import jax
import jax.numpy as jnp
from jax import lax

ROWS = 1024
D = 7168
HEADS = 56
KV_HEADS = 56
HEAD = 128
THETA = 10000


def setup_inputs(seed: int = 0, part: int = 0) -> dict:
    kx, kn, kq, kk, kv, ko = jax.random.split(jax.random.key(seed), 6)

    def weights(key, rows, columns):
        return jax.random.normal(key, (rows, columns), jnp.float32) * rows**-0.5

    drawn = {
        "x": jax.random.normal(jax.random.fold_in(kx, part), (ROWS, D), jnp.float32),
        "gain": 1 + 0.1 * jax.random.normal(kn, (D,), jnp.float32),
        "wq": 2 * weights(kq, D, HEADS * HEAD),
        "wk": 2 * weights(kk, D, KV_HEADS * HEAD),
        "wv": 4 * weights(kv, D, KV_HEADS * HEAD),
        "wo": weights(ko, HEADS * HEAD, D),
    }
    return {k: v.astype(jnp.bfloat16) for k, v in drawn.items()}


def normed(x, gain):
    wide = x.astype(jnp.float32)
    scale = lax.rsqrt(jnp.mean(wide * wide, -1, keepdims=True) + 1e-6)
    return (wide * scale * gain.astype(jnp.float32)).astype(jnp.bfloat16)


def turned(t, place, theta):
    half = t.shape[-1] // 2
    angle = place.astype(jnp.float32)[:, None] * theta ** (-jnp.arange(half, dtype=jnp.float32) / half)
    cos, sin = jnp.cos(angle)[:, None], jnp.sin(angle)[:, None]
    a, b = t[..., :half].astype(jnp.float32), t[..., half:].astype(jnp.float32)
    return jnp.concatenate([a * cos - b * sin, b * cos + a * sin], -1).astype(jnp.bfloat16)


def matmul(a, w):
    return jnp.dot(a, w, preferred_element_type=jnp.float32).astype(jnp.bfloat16)


def einsum(form, a, b):
    return jnp.einsum(form, a.astype(jnp.float32), b.astype(jnp.float32))


def attention(q, k, v):
    scores = einsum("tgsd,ugd->gstu", q, k) * q.shape[-1] ** -0.5
    token = jnp.arange(q.shape[0])
    scores = jnp.where(token[:, None] >= token, scores, -jnp.inf)
    weights = jax.nn.softmax(scores, -1).astype(jnp.bfloat16)
    return einsum("gstu,ugd->tgsd", weights, v).astype(jnp.bfloat16)


def reference(x, gain, wq, wk, wv, wo):
    a, place = normed(x, gain), jnp.arange(ROWS)
    q = turned(matmul(a, wq).reshape(ROWS, HEADS, HEAD), place, THETA).reshape(ROWS, KV_HEADS, -1, HEAD)
    k = turned(matmul(a, wk).reshape(ROWS, KV_HEADS, HEAD), place, THETA)
    v = matmul(a, wv).reshape(ROWS, KV_HEADS, HEAD)
    seen = attention(q, k, v).reshape(ROWS, HEADS * HEAD)
    return (x.astype(jnp.float32) + jnp.dot(seen, wo, preferred_element_type=jnp.float32)).astype(jnp.bfloat16)
```

```python
import functools

import jax
import jax.numpy as jnp
import numpy as np
from jax import lax
from jax.experimental import pallas as pl
from jax.experimental.pallas import tpu as pltpu
from jax.sharding import PartitionSpec as P

HEAD = 128
THETA = 10000
SLICE = 512
KEYS = 256
NEG = -1e30
HIDDEN = 2 * NEG
LOG2E = 1.4426950408889634
MESH = pl.DeviceIdType.MESH
AUG = HEAD + 16


def dot(a, b, ca=1, cb=0):
    return lax.dot_general(a, b, (((ca,), (cb,)), ((), ())), preferred_element_type=jnp.float32)


def kernel(n, x_ref, gain_ref, cos_ref, sin_ref, wq_ref, wk_ref, wv_ref, wo_ref, y_ref, buf, wb, acc, qb, kb, vt, wob, ob, term, top_s, mix_s,
           send_sem, recv_sem, w_sem, wo_sem, x_sem, y_sem):
    me = lax.axis_index("tp")
    right, left = lax.rem(me + 1, n), lax.rem(me + n - 1, n)
    slices, rows = buf.shape[1], buf.shape[2]
    half = rows // 2
    depth = x_ref.shape[1]
    columns = wq_ref.shape[1]
    heads = columns // HEAD
    group = mix_s.shape[0]
    groups = heads // group
    wos = wob.shape[0]
    halves = (pl.ds(0, half), pl.ds(half, half))
    total = n * slices

    def lanes(c, width=SLICE):
        return pl.ds(pl.multiple_of(c * width, width), width)

    def hop(way, k, s):
        return pltpu.make_async_remote_copy(
            src_ref=buf.at[k, s, halves[way]],
            dst_ref=buf.at[k + 1, s, halves[way]],
            send_sem=send_sem.at[way, k, s],
            recv_sem=recv_sem.at[way, k, s],
            device_id={"tp": left if way else right},
            device_id_type=MESH,
        )

    def weights(t, m):
        w = (wq_ref, wk_ref, wv_ref)[m]
        s, slot = lax.rem(t, slices), lax.rem(t, 2)
        return pltpu.make_async_copy(w.at[pl.ds(pl.multiple_of(s * SLICE, SLICE), SLICE)], wb.at[slot, m], w_sem.at[slot, m])

    def out_weights(t):
        slot = lax.rem(t, wos)
        return pltpu.make_async_copy(wo_ref.at[:, lanes(lax.rem(t, slices))], wob.at[slot], wo_sem.at[slot])

    def x_slice(s):
        return pltpu.make_async_copy(x_ref.at[:, lanes(s)], buf.at[0, s], x_sem.at[s])

    def y_slice(s):
        return pltpu.make_async_copy(buf.at[1, s], y_ref.at[:, lanes(s)], y_sem.at[s])

    def place(h, side):
        return pl.multiple_of((1 - side) * (lax.rem(me - h + n, n) * rows) + side * (lax.rem(me + h, n) * rows + half), half)

    barrier = pltpu.get_barrier_semaphore()
    for neighbour in (left, right):
        pl.semaphore_signal(barrier, inc=1, device_id={"tp": neighbour}, device_id_type=MESH)
    for s in range(slices):
        x_slice(s).start()
    for t in range(2):
        for m in range(3):
            weights(t, m).start()
    acc[...] = jnp.zeros_like(acc)
    vt[:, HEAD:, :] = jnp.ones((heads, AUG - HEAD, vt.shape[2]), vt.dtype)

    def square(s, sums):
        x_slice(s).wait()
        wide = buf[0, s].astype(jnp.float32)
        wide = wide * wide
        for at in range(0, SLICE, 128):
            sums = sums + wide[:, at : at + 128]
        return sums

    sums = lax.fori_loop(0, slices, square, jnp.zeros((rows, 128), jnp.float32))
    scale = lax.rsqrt(jnp.sum(sums, axis=1, keepdims=True) * (1 / depth) + 1e-6)
    pl.semaphore_wait(barrier, 2)

    def norm(s, _):
        buf[0, s] = (buf[0, s].astype(jnp.float32) * scale * gain_ref[:, lanes(s)].astype(jnp.float32)).astype(buf.dtype)

        @pl.when(s > 0)
        def _():
            for way in range(2):
                hop(way, 0, s - 1).start()

    lax.fori_loop(0, slices, norm, None)
    for way in range(2):
        hop(way, 0, slices - 1).start()

    def turn(h):
        def side_of(side, _):
            at = place(h, side)
            mine = pl.ds(pl.multiple_of(side * half, half), half)
            here = pl.ds(at, half)
            cos, sin = cos_ref[here, :], sin_ref[here, :]
            for i in range(heads):
                head = slice(i * HEAD, (i + 1) * HEAD)
                for m, to in ((0, qb), (1, kb)):
                    v = acc[m, mine, head].astype(jnp.bfloat16).astype(jnp.float32)
                    to[here, head] = (v * cos + pltpu.roll(v, HEAD // 2, axis=1) * sin).astype(to.dtype)
                vt[i, :HEAD, here] = acc[2, mine, head].T.astype(vt.dtype)

        lax.fori_loop(0, 2, side_of, None)
        acc[...] = jnp.zeros_like(acc)

    def project(t, _):
        h, s = lax.div(t, slices), lax.rem(t, slices)
        slot = lax.rem(t, 2)

        @pl.when(h > 0)
        def _():
            for way in range(2):
                hop(way, h - 1, s).wait_recv()

        @pl.when((h > 0) & (h < n - 1))
        def _():
            for way in range(2):
                hop(way, h, s).start()

        for m in range(3):
            weights(t, m).wait()
            acc[m] += dot(buf[h, s], wb[slot, m])

            @pl.when(t + 2 < total)
            def _():
                weights(t + 2, m).start()

        @pl.when(s == slices - 1)
        def _():
            turn(h)

    for t in range(wos):
        out_weights(t).start()
    lax.fori_loop(0, total, project, None)

    def sent(k):
        def one(s, _):
            for way in range(2):
                hop(way, k, s).wait_send()

        lax.fori_loop(0, slices, one, None)

    sent(0)
    sent(1)
    for s in range(slices):
        x_slice(s).start()

    e = HEAD**-0.5 * LOG2E

    def attend(i):
        def part(p, _):
            side, g = lax.div(p, groups), lax.rem(p, groups)
            at = place(i, side)
            here = pl.ds(at, half)
            first = g * group

            def head(u):
                return pl.ds(pl.multiple_of((first + u) * HEAD, HEAD), HEAD)

            for u in range(group):
                top_s[u] = jnp.full((1, half), NEG, jnp.float32)
                mix_s[u] = jnp.zeros((AUG, half), jnp.float32)

            def block(j, masked):
                keys = pl.ds(pl.multiple_of(j * KEYS, KEYS), KEYS)
                scores = [dot(kb[keys, head(u)], qb[here, head(u)], 1, 1) for u in range(group)]
                if masked:
                    gap = lax.broadcasted_iota(jnp.int32, (KEYS, half), 1) - lax.broadcasted_iota(jnp.int32, (KEYS, half), 0)
                    seen = gap >= j * KEYS - at
                tops, ps = [], []
                for u in range(group):
                    s = jnp.where(seen, scores[u], HIDDEN) if masked else scores[u]
                    old = top_s[u]
                    top = jnp.maximum(old, s.max(axis=0, keepdims=True))
                    top_s[u] = top
                    ps.append(jnp.exp2((s - top) * e).astype(jnp.bfloat16))
                    tops.append(jnp.exp2((old - top) * e))
                for u in range(group):
                    mix_s[u] = mix_s[u] * tops[u] + dot(vt[first + u, :, keys], ps[u])

            whole = lax.div(at, KEYS)
            lax.fori_loop(0, whole, lambda j, _: block(j, False), None)
            block(whole, True)
            for u in range(group):
                weight = 1 / mix_s[u, HEAD : HEAD + 1, :]
                ob[pl.ds(pl.multiple_of(side * half, half), half), head(u)] = (mix_s[u, :HEAD, :] * weight).T.astype(ob.dtype)

        lax.fori_loop(0, 2 * groups, part, None)

    def step(i, _):
        attend(i)
        k = n - 2 + i

        def chunk(c, _):
            t = (i - 1) * slices + c
            out_weights(t).wait()
            term[...] = dot(ob[...], wob[lax.rem(t, wos)])

            @pl.when(t + wos < total)
            def _():
                out_weights(t + wos).start()

            @pl.when((c > 0) & (i < n))
            def _():
                for way in range(2):
                    hop(way, k, c - 1).start()

            @pl.when(i > 1)
            def _():
                for way in range(2):
                    hop(way, k - 1, c).wait_recv()
                term[...] += buf[k, c].astype(jnp.float32)

            @pl.when(i < n)
            def _():
                buf[k, c] = term[...].astype(buf.dtype)

            @pl.when(i == n)
            def _():
                x_slice(c).wait()
                buf[1, c] = (buf[0, c].astype(jnp.float32) + term[...]).astype(buf.dtype)

                @pl.when(c > 0)
                def _():
                    y_slice(c - 1).start()

        lax.fori_loop(0, slices, chunk, None)

        @pl.when(i < n)
        def _():
            for way in range(2):
                hop(way, k, slices - 1).start()

    lax.fori_loop(1, n + 1, step, None)
    y_slice(slices - 1).start()
    for k in range(2, 2 * n - 2):
        sent(k)
    for s in range(slices):
        y_slice(s).wait()


def tables(tokens):
    half = HEAD // 2
    power = np.power(np.float32(THETA), -np.arange(half, dtype=np.float32) / np.float32(half)).astype(np.float32)
    angle = np.arange(tokens, dtype=np.float32)[:, None] * power
    cos, sin = np.cos(angle).astype(np.float32), np.sin(angle).astype(np.float32)
    return np.concatenate([cos, cos], 1), np.concatenate([-sin, sin], 1)


def solution(mesh):
    n = mesh.shape["tp"]

    def step(x, gain, wq, wk, wv, wo):
        rows, depth = x.shape
        columns = wq.shape[1]
        heads = columns // HEAD
        group = heads // 2
        slices = depth // SLICE
        tokens = n * rows
        bf16, f32 = jnp.bfloat16, jnp.float32
        cos, sin = tables(tokens)
        whole = pl.BlockSpec(memory_space=pltpu.VMEM)
        hbm = pl.BlockSpec(memory_space=pl.ANY)
        return pl.pallas_call(
            functools.partial(kernel, n),
            out_shape=jax.ShapeDtypeStruct((rows, depth), bf16),
            in_specs=[hbm, whole, whole, whole, hbm, hbm, hbm, hbm],
            out_specs=hbm,
            scratch_shapes=[
                pltpu.VMEM((2 * n - 1, slices, rows, SLICE), bf16),
                pltpu.VMEM((2, 3, SLICE, columns), bf16),
                pltpu.VMEM((3, rows, columns), f32),
                pltpu.VMEM((tokens, columns), bf16),
                pltpu.VMEM((tokens, columns), bf16),
                pltpu.VMEM((heads, AUG, tokens), bf16),
                pltpu.VMEM((2, columns, SLICE), bf16),
                pltpu.VMEM((rows, columns), bf16),
                pltpu.VMEM((rows, SLICE), f32),
                pltpu.VMEM((group, 1, rows // 2), f32),
                pltpu.VMEM((group, AUG, rows // 2), f32),
                pltpu.SemaphoreType.DMA((2, 2 * n - 2, slices)),
                pltpu.SemaphoreType.DMA((2, 2 * n - 2, slices)),
                pltpu.SemaphoreType.DMA((2, 3)),
                pltpu.SemaphoreType.DMA((2,)),
                pltpu.SemaphoreType.DMA((slices,)),
                pltpu.SemaphoreType.DMA((slices,)),
            ],
            compiler_params=pltpu.CompilerParams(collective_id=0, has_side_effects=True, vmem_limit_bytes=67_000_000),
        )(x, gain.reshape(1, -1), cos, sin, wq, wk, wv, wo)

    tokens, columns = P(("dp", "tp"), None), P(None, "tp")
    return jax.shard_map(
        step,
        mesh=mesh,
        in_specs=(tokens, P(None), columns, columns, columns, P("tp", None)),
        out_specs=tokens,
        check_vma=False,
    )
```

```python
import functools

import jax
import jax.numpy as jnp
import numpy as np
from jax import lax
from jax.experimental import pallas as pl
from jax.experimental.pallas import tpu as pltpu
from jax.sharding import PartitionSpec as P

HEAD = 128
THETA = 10000
SLICE = 512
KEYS = 256
NEG = -1e30
HIDDEN = 2 * NEG
LOG2E = 1.4426950408889634
MESH = pl.DeviceIdType.MESH
ORDER = (1, 2, 0)
AUG = HEAD + 16


def dot(a, b, ca=1, cb=0):
    return lax.dot_general(a, b, (((ca,), (cb,)), ((), ())), preferred_element_type=jnp.float32)


def kernel(n, group, x_ref, gain_ref, angle_ref, wq_ref, wk_ref, wv_ref, wo_ref, y_ref, buf, wb, acc, qb, kb, vt, wob, ob, tab, term, top_e, mix_e,
           send_sem, recv_sem, w_sem, wo_sem, x_sem, tab_sem):
    me = lax.axis_index("tp")
    right, left = lax.rem(me + 1, n), lax.rem(me + n - 1, n)
    slices, rows = buf.shape[1], buf.shape[2]
    half = rows // 2
    depth = x_ref.shape[1]
    columns = wq_ref.shape[1]
    heads = columns // HEAD
    groups = heads // group
    wos = wob.shape[0]
    halves = (pl.ds(0, half), pl.ds(half, half))
    total = n * slices
    share = -(-heads // slices)
    e = HEAD**-0.5 * LOG2E

    def lanes(c, width=SLICE):
        return pl.ds(pl.multiple_of(c * width, width), width)

    def hop(way, k, s):
        return pltpu.make_async_remote_copy(
            src_ref=buf.at[k, s, halves[way]],
            dst_ref=buf.at[k + 1, s, halves[way]],
            send_sem=send_sem.at[way, k, s],
            recv_sem=recv_sem.at[way, k, s],
            device_id={"tp": left if way else right},
            device_id_type=MESH,
        )

    def weights(t, m):
        w = (wq_ref, wk_ref, wv_ref)[m]
        s, slot = lax.rem(t, slices), lax.rem(t, 2)
        return pltpu.make_async_copy(w.at[pl.ds(pl.multiple_of(s * SLICE, SLICE), SLICE)], wb.at[slot, m], w_sem.at[slot, m])

    def out_weights(t):
        slot = lax.rem(t, wos)
        return pltpu.make_async_copy(wo_ref.at[:, lanes(lax.rem(t, slices))], wob.at[slot], wo_sem.at[slot])

    def x_slice(s):
        return pltpu.make_async_copy(x_ref.at[:, lanes(s)], buf.at[0, s], x_sem.at[s])

    def y_slice(s):
        return pltpu.make_async_copy(buf.at[1, s], y_ref.at[:, lanes(s)], x_sem.at[s])

    def place(h, side):
        return pl.multiple_of((1 - side) * (lax.rem(me - h + n, n) * rows) + side * (lax.rem(me + h, n) * rows + half), half)

    def angles(h, side):
        return pltpu.make_async_copy(angle_ref.at[pl.ds(place(h, side), half)], tab.at[side], tab_sem.at[side])

    barrier = pltpu.get_barrier_semaphore()
    for neighbour in (left, right):
        pl.semaphore_signal(barrier, inc=1, device_id={"tp": neighbour}, device_id_type=MESH)
    for s in range(slices):
        x_slice(s).start()
    acc[...] = jnp.zeros_like(acc)
    vt[:, HEAD:, :] = jnp.ones((heads, AUG - HEAD, vt.shape[2]), vt.dtype)

    def square(s, sums):
        x_slice(s).wait()
        wide = buf[0, s].astype(jnp.float32)
        wide = wide * wide
        for at in range(0, SLICE, 128):
            sums = sums + wide[:, at : at + 128]
        return sums

    sums = lax.fori_loop(0, slices, square, jnp.zeros((rows, 128), jnp.float32))
    for t in range(2):
        for m in ORDER:
            weights(t, m).start()
    scale = lax.rsqrt(jnp.sum(sums, axis=1, keepdims=True) * (1 / depth) + 1e-6)
    pl.semaphore_wait(barrier, 2)

    def norm(s, _):
        buf[0, s] = (buf[0, s].astype(jnp.float32) * scale * gain_ref[:, lanes(s)]).astype(buf.dtype)

        @pl.when(s > 0)
        def _():
            for way in range(2):
                hop(way, 0, s - 1).start()

    lax.fori_loop(0, slices, norm, None)
    for way in range(2):
        hop(way, 0, slices - 1).start()

    def turn(h, parts):
        def side_of(side, _):
            mine = pl.ds(pl.multiple_of(side * half, half), half)
            here = pl.ds(place(h, side), half)
            both = tab[side]
            other = pltpu.roll(both, HEAD // 2, axis=1)
            low = lax.broadcasted_iota(jnp.int32, both.shape, 1) < HEAD // 2
            cos, sin = jnp.where(low, both, other), jnp.where(low, -other, both)
            for i in range(heads):
                head = slice(i * HEAD, (i + 1) * HEAD)
                for m in parts:
                    if m == 2:
                        vt[i, :HEAD, here] = acc[m, mine, head].T.astype(vt.dtype)
                    else:
                        v = acc[m, mine, head].astype(jnp.bfloat16).astype(jnp.float32)
                        (qb, kb)[m][here, head] = (v * cos + pltpu.roll(v, HEAD // 2, axis=1) * sin).astype(kb.dtype)

        lax.fori_loop(0, 2, side_of, None)

    def product(t, m):
        weights(t, m).wait()
        acc[m] += dot(buf[lax.div(t, slices), lax.rem(t, slices)], wb[lax.rem(t, 2), m])

    def early(i):
        head = pl.ds(pl.multiple_of(i * HEAD, HEAD), HEAD)
        gap = lax.broadcasted_iota(jnp.int32, (half, half), 1) - lax.broadcasted_iota(jnp.int32, (half, half), 0)
        known = [place(h, side) for h in range(n - 1) for side in range(2)]
        all_scores = []
        for side in range(2):
            at = place(1, side)
            q = qb[pl.ds(at, half), head]
            all_scores.append([jnp.where(gap >= k - at, dot(kb[pl.ds(k, half), head], q, 1, 1), HIDDEN) for k in known])
        for side in range(2):
            scores = all_scores[side]
            top = functools.reduce(jnp.maximum, scores).max(axis=0, keepdims=True)
            top_e[side, i] = top
            mix_e[side, i] = sum(dot(vt[i, :, pl.ds(k, half)], jnp.exp2((s - top) * e).astype(jnp.bfloat16)) for k, s in zip(known, scores))

    def project(t, _):
        h, s = lax.div(t, slices), lax.rem(t, slices)

        @pl.when(h > 0)
        def _():
            for way in range(2):
                hop(way, h - 1, s).wait_recv()

        @pl.when((h > 0) & (h < n - 1))
        def _():
            for way in range(2):
                hop(way, h, s).start()

        for m in ORDER[:2]:
            product(t, m)

            @pl.when(t + 2 < total)
            def _():
                weights(t + 2, m).start()

        @pl.when(t < total - 1)
        def _():
            product(t, 0)

            @pl.when(t + 2 < total)
            def _():
                weights(t + 2, 0).start()

        @pl.when(h == n - 1)
        def _():
            for u in range(share):

                @pl.when(s * share + u < heads)
                def _():
                    early(s * share + u)

        @pl.when(s == 0)
        def _():
            for side in range(2):
                angles(h, side).start()

        @pl.when(s == slices - 1)
        def _():
            for side in range(2):
                angles(h, side).wait()

        @pl.when((s == slices - 1) & (h < n - 1))
        def _():
            turn(h, (0, 1, 2))
            acc[...] = jnp.zeros_like(acc)

    for t in range(wos):
        out_weights(t).start()
    lax.fori_loop(0, total, project, None)

    turn(n - 1, (1, 2))

    def sent(k):
        def one(s, _):
            for way in range(2):
                hop(way, k, s).wait_send()

        lax.fori_loop(0, slices, one, None)

    def late():
        def pair(p, _):
            side, other, first = lax.div(p, 2 * groups), lax.rem(p, 2), lax.rem(lax.div(p, 2), groups) * group
            at, k = place(1, side), place(n - 1, other)
            here, keys = pl.ds(at, half), pl.ds(k, half)

            @pl.when(k < at)
            def _():
                heads_here = [pl.ds(pl.multiple_of((first + u) * HEAD, HEAD), HEAD) for u in range(group)]
                scores = [dot(kb[keys, head], qb[here, head], 1, 1) for head in heads_here]
                ps, keeps = [], []
                for u, s in enumerate(scores):
                    old = top_e[side, first + u]
                    top = jnp.maximum(old, s.max(axis=0, keepdims=True))
                    top_e[side, first + u] = top
                    ps.append(jnp.exp2((s - top) * e).astype(jnp.bfloat16))
                    keeps.append(jnp.exp2((old - top) * e))
                for u in range(group):
                    mix_e[side, first + u] = mix_e[side, first + u] * keeps[u] + dot(vt[first + u, :, keys], ps[u])

        lax.fori_loop(0, 4 * groups, pair, None)

        def done(side, _):
            for i in range(heads):
                weight = 1 / mix_e[side, i, HEAD : HEAD + 1, :]
                out = (mix_e[side, i, :HEAD, :] * weight).T.astype(ob.dtype)
                ob[pl.ds(pl.multiple_of(side * half, half), half), i * HEAD : (i + 1) * HEAD] = out

        lax.fori_loop(0, 2, done, None)

    def attend(i):
        def part(p, _):
            side, g = lax.div(p, groups), lax.rem(p, groups)
            at = place(i, side)
            here = pl.ds(at, half)
            first = g * group

            def head(u):
                return pl.ds(pl.multiple_of((first + u) * HEAD, HEAD), HEAD)

            for u in range(group):
                top_e[0, u] = jnp.full((1, half), NEG, jnp.float32)
                mix_e[0, u] = jnp.zeros((AUG, half), jnp.float32)

            def block(j, masked):
                keys = pl.ds(pl.multiple_of(j * KEYS, KEYS), KEYS)
                scores = [dot(kb[keys, head(u)], qb[here, head(u)], 1, 1) for u in range(group)]
                if masked:
                    gap = lax.broadcasted_iota(jnp.int32, (KEYS, half), 1) - lax.broadcasted_iota(jnp.int32, (KEYS, half), 0)
                    seen = gap >= j * KEYS - at
                tops, ps = [], []
                for u in range(group):
                    s = jnp.where(seen, scores[u], HIDDEN) if masked else scores[u]
                    old = top_e[0, u]
                    top = jnp.maximum(old, s.max(axis=0, keepdims=True))
                    top_e[0, u] = top
                    ps.append(jnp.exp2((s - top) * e).astype(jnp.bfloat16))
                    tops.append(jnp.exp2((old - top) * e))
                for u in range(group):
                    mix_e[0, u] = mix_e[0, u] * tops[u] + dot(vt[first + u, :, keys], ps[u])

            whole = lax.div(at, KEYS)
            lax.fori_loop(0, whole, lambda j, _: block(j, False), None)
            block(whole, True)
            for u in range(group):
                weight = 1 / mix_e[0, u, HEAD : HEAD + 1, :]
                ob[pl.ds(pl.multiple_of(side * half, half), half), head(u)] = (mix_e[0, u, :HEAD, :] * weight).T.astype(ob.dtype)

        lax.fori_loop(0, 2 * groups, part, None)

    def step(i, _):
        @pl.when(i == 1)
        def _():
            late()

        @pl.when(i == 2)
        def _():
            turn(n - 1, (0,))
            sent(0)
            sent(1)
            for s in range(slices):
                x_slice(s).start()

        @pl.when(i > 1)
        def _():
            attend(i)

        k = n - 2 + i

        def ship(c):
            @pl.when(i < n)
            def _():
                for way in range(2):
                    hop(way, k, c).start()

        def chunk(c, _):
            t = (i - 1) * slices + c
            out_weights(t).wait()
            term[...] = dot(ob[...], wob[lax.rem(t, wos)])

            @pl.when(t + wos < total)
            def _():
                out_weights(t + wos).start()

            @pl.when(c > 0)
            def _():
                ship(c - 1)

            @pl.when((i == 1) & (c == slices - 2))
            def _():
                product(total - 1, 0)

            @pl.when(i > 1)
            def _():
                for way in range(2):
                    hop(way, k - 1, c).wait_recv()
                term[...] += buf[k, c].astype(jnp.float32)

            @pl.when(i < n)
            def _():
                buf[k, c] = term[...].astype(buf.dtype)

            @pl.when(i == n)
            def _():
                x_slice(c).wait()
                buf[1, c] = (buf[0, c].astype(jnp.float32) + term[...]).astype(buf.dtype)

                @pl.when(c > 0)
                def _():
                    y_slice(c - 1).start()

        lax.fori_loop(0, slices, chunk, None)

        ship(slices - 1)

    lax.fori_loop(1, n + 1, step, None)
    y_slice(slices - 1).start()
    for k in range(2, 2 * n - 2):
        sent(k)
    for s in range(slices):
        y_slice(s).wait()


def tables(tokens):
    half = HEAD // 2
    power = np.power(np.float32(THETA), -np.arange(half, dtype=np.float32) / np.float32(half)).astype(np.float32)
    angle = np.arange(tokens, dtype=np.float32)[:, None] * power
    return np.concatenate([np.cos(angle), np.sin(angle)], 1).astype(np.float32)


def solution(mesh):
    n = mesh.shape["tp"]

    def step(x, gain, wq, wk, wv, wo):
        rows, depth = x.shape
        columns = wq.shape[1]
        heads = columns // HEAD
        slices = depth // SLICE
        tokens = n * rows
        bf16, f32 = jnp.bfloat16, jnp.float32
        whole = pl.BlockSpec(memory_space=pltpu.VMEM)
        hbm = pl.BlockSpec(memory_space=pl.ANY)
        return pl.pallas_call(
            functools.partial(kernel, n, heads // 2),
            out_shape=jax.ShapeDtypeStruct((rows, depth), bf16),
            in_specs=[hbm, whole, hbm, hbm, hbm, hbm, hbm],
            out_specs=hbm,
            scratch_shapes=[
                pltpu.VMEM((2 * n - 1, slices, rows, SLICE), bf16),
                pltpu.VMEM((2, 3, SLICE, columns), bf16),
                pltpu.VMEM((3, rows, columns), f32),
                pltpu.VMEM((tokens, columns), bf16),
                pltpu.VMEM((tokens, columns), bf16),
                pltpu.VMEM((heads, AUG, tokens), bf16),
                pltpu.VMEM((2, columns, SLICE), bf16),
                pltpu.VMEM((rows, columns), bf16),
                pltpu.VMEM((2, rows // 2, HEAD), f32),
                pltpu.VMEM((rows, SLICE), f32),
                pltpu.VMEM((2, heads, 1, rows // 2), f32),
                pltpu.VMEM((2, heads, AUG, rows // 2), f32),
                pltpu.SemaphoreType.DMA((2, 2 * n - 2, slices)),
                pltpu.SemaphoreType.DMA((2, 2 * n - 2, slices)),
                pltpu.SemaphoreType.DMA((2, 3)),
                pltpu.SemaphoreType.DMA((2,)),
                pltpu.SemaphoreType.DMA((slices,)),
                pltpu.SemaphoreType.DMA((2,)),
            ],
            compiler_params=pltpu.CompilerParams(collective_id=0, has_side_effects=True, vmem_limit_bytes=67_000_000),
        )(x, gain.astype(f32).reshape(1, -1), tables(tokens), wq, wk, wv, wo)

    tokens, columns = P(("dp", "tp"), None), P(None, "tp")
    return jax.shard_map(
        step,
        mesh=mesh,
        in_specs=(tokens, P(None), columns, columns, columns, P("tp", None)),
        out_specs=tokens,
        check_vma=False,
    )
```

```python
import functools

import jax
import jax.numpy as jnp
import numpy as np
from jax import lax
from jax.experimental import pallas as pl
from jax.experimental.pallas import tpu as pltpu
from jax.sharding import PartitionSpec as P

HEAD = 128
THETA = 10000
SLICE = 512
KEYS = 256
NEG = -1e30
HIDDEN = 2 * NEG
LOG2E = 1.4426950408889634
MESH = pl.DeviceIdType.MESH
ORDER = (1, 2, 0)
AUG = HEAD + 16


def dot(a, b, ca=1, cb=0):
    return lax.dot_general(a, b, (((ca,), (cb,)), ((), ())), preferred_element_type=jnp.float32)


def kernel(n, group, x_ref, gain_ref, angle_ref, wq_ref, wk_ref, wv_ref, wo_ref, y_ref, buf, wb, acc, qb, kb, vt, wob, ob, term, top_e, mix_e,
           send_sem, recv_sem, w_sem, wo_sem, x_sem):
    me = lax.axis_index("tp")
    right, left = lax.rem(me + 1, n), lax.rem(me + n - 1, n)
    slices, rows = buf.shape[1], buf.shape[2]
    half = rows // 2
    depth = x_ref.shape[1]
    columns = wq_ref.shape[1]
    heads = columns // HEAD
    groups = heads // group
    wos = wob.shape[0]
    halves = (pl.ds(0, half), pl.ds(half, half))
    total = n * slices
    share = -(-heads // slices)
    e = HEAD**-0.5 * LOG2E

    def lanes(c, width=SLICE):
        return pl.ds(pl.multiple_of(c * width, width), width)

    def hop(way, k, s, source=None):
        return pltpu.make_async_remote_copy(
            src_ref=buf.at[k if source is None else source, s, halves[way]],
            dst_ref=buf.at[k + 1, s, halves[way]],
            send_sem=send_sem.at[way, k, s],
            recv_sem=recv_sem.at[way, k, s],
            device_id={"tp": left if way else right},
            device_id_type=MESH,
        )

    def weights(t, m):
        w = (wq_ref, wk_ref, wv_ref)[m]
        s, slot = lax.rem(t, slices), lax.rem(t, 2)
        return pltpu.make_async_copy(w.at[pl.ds(pl.multiple_of(s * SLICE, SLICE), SLICE)], wb.at[slot, m], w_sem.at[slot, m])

    def out_weights(t):
        slot = lax.rem(t, wos)
        return pltpu.make_async_copy(wo_ref.at[:, lanes(lax.rem(t, slices))], wob.at[slot], wo_sem.at[slot])

    def x_slice(s):
        return pltpu.make_async_copy(x_ref.at[:, lanes(s)], buf.at[0, s], x_sem.at[s])

    def y_slice(s):
        return pltpu.make_async_copy(buf.at[2, s], y_ref.at[:, lanes(s)], x_sem.at[s])

    def place(h, side):
        return pl.multiple_of((1 - side) * (lax.rem(me - h + n, n) * rows) + side * (lax.rem(me + h, n) * rows + half), half)

    barrier = pltpu.get_barrier_semaphore()
    for neighbour in (left, right):
        pl.semaphore_signal(barrier, inc=1, device_id={"tp": neighbour}, device_id_type=MESH)
    for s in range(slices):
        x_slice(s).start()
    acc[...] = jnp.zeros_like(acc)
    vt[:, HEAD:, :] = jnp.ones((heads, AUG - HEAD, vt.shape[2]), vt.dtype)

    def square(s, sums):
        x_slice(s).wait()
        wide = buf[0, s].astype(jnp.float32)
        wide = wide * wide
        for at in range(0, SLICE, 128):
            sums = sums + wide[:, at : at + 128]
        return sums

    sums = lax.fori_loop(0, slices, square, jnp.zeros((rows, 128), jnp.float32))
    for t in range(2):
        for m in ORDER:
            weights(t, m).start()
    scale = lax.rsqrt(jnp.sum(sums, axis=1, keepdims=True) * (1 / depth) + 1e-6)
    pl.semaphore_wait(barrier, 2)

    def norm(s, _):
        buf[0, s] = (buf[0, s].astype(jnp.float32) * scale * gain_ref[:, lanes(s)]).astype(buf.dtype)

        @pl.when(s > 0)
        def _():
            for way in range(2):
                hop(way, 0, s - 1).start()

    lax.fori_loop(0, slices, norm, None)
    for way in range(2):
        hop(way, 0, slices - 1).start()

    def turn(h, parts):
        def side_of(side, _):
            mine = pl.ds(pl.multiple_of(side * half, half), half)
            here = pl.ds(place(h, side), half)
            both = angle_ref[here, :]
            other = pltpu.roll(both, HEAD // 2, axis=1)
            low = lax.broadcasted_iota(jnp.int32, both.shape, 1) < HEAD // 2
            cos, sin = jnp.where(low, both, other), jnp.where(low, -other, both)
            for i in range(heads):
                head = slice(i * HEAD, (i + 1) * HEAD)
                for m, held in parts:
                    if m == 2:
                        vt[i, :HEAD, here] = acc[held, mine, head].T.astype(vt.dtype)
                    else:
                        v = acc[held, mine, head].astype(jnp.bfloat16).astype(jnp.float32)
                        (qb, kb)[m][here, head] = (v * cos + pltpu.roll(v, HEAD // 2, axis=1) * sin).astype(kb.dtype)

        lax.fori_loop(0, 2, side_of, None)

    def product(h, t, m):
        weights(t, m).wait()
        acc[m] += dot(buf[h, lax.rem(t, slices)], wb[lax.rem(t, 2), m])

    def early(i):
        head = pl.ds(pl.multiple_of(i * HEAD, HEAD), HEAD)
        gap = lax.broadcasted_iota(jnp.int32, (half, half), 1) - lax.broadcasted_iota(jnp.int32, (half, half), 0)
        known = [place(h, side) for h in range(n - 1) for side in range(2)]
        all_scores = []
        for side in range(2):
            at = place(1, side)
            q = qb[pl.ds(at, half), head]
            all_scores.append([jnp.where(gap >= k - at, dot(kb[pl.ds(k, half), head], q, 1, 1), HIDDEN) for k in known])
        for side in range(2):
            scores = all_scores[side]
            top = functools.reduce(jnp.maximum, scores).max(axis=0, keepdims=True)
            top_e[side, i] = top
            mix_e[side, i] = sum(dot(vt[i, :, pl.ds(k, half)], jnp.exp2((s - top) * e).astype(jnp.bfloat16)) for k, s in zip(known, scores))

    def project(t, _):
        h, s = lax.div(t, slices), lax.rem(t, slices)

        @pl.when(h > 0)
        def _():
            for way in range(2):
                hop(way, h - 1, s).wait_recv()

        @pl.when((h > 0) & (h < n - 1))
        def _():
            for way in range(2):
                hop(way, h, s).start()

        for m in (1, 2):
            product(h, t, m)

            @pl.when(t + 2 < total)
            def _():
                weights(t + 2, m).start()

        @pl.when(h == 1)
        def _():
            product(1, s, 0)
            weights(s + 2, 0).start()

        @pl.when(h == n - 1)
        def _():
            for u in range(share):

                @pl.when(s * share + u < heads)
                def _():
                    early(s * share + u)

        @pl.when((s == slices - 1) & (h < n - 1))
        def _():
            turn(h, ((1, 1), (2, 2)))
            acc[1:3] = jnp.zeros((2, *acc.shape[1:]), acc.dtype)

        @pl.when((s == slices - 1) & (h == 1))
        def _():
            turn(1, ((0, 0),))

    def sent(k):
        def one(s, _):
            for way in range(2):
                hop(way, k, s).wait_send()

        lax.fori_loop(0, slices, one, None)

    for t in range(wos):
        out_weights(t).start()
    lax.fori_loop(0, total, project, None)

    turn(n - 1, ((1, 1), (2, 2)))
    sent(1)

    def late():
        def pair(p, _):
            side, other, first = lax.div(p, 2 * groups), lax.rem(p, 2), lax.rem(lax.div(p, 2), groups) * group
            at, k = place(1, side), place(n - 1, other)
            here, keys = pl.ds(at, half), pl.ds(k, half)

            @pl.when(k < at)
            def _():
                heads_here = [pl.ds(pl.multiple_of((first + u) * HEAD, HEAD), HEAD) for u in range(group)]
                scores = [dot(kb[keys, head], qb[here, head], 1, 1) for head in heads_here]
                ps, keeps = [], []
                for u, s in enumerate(scores):
                    old = top_e[side, first + u]
                    top = jnp.maximum(old, s.max(axis=0, keepdims=True))
                    top_e[side, first + u] = top
                    ps.append(jnp.exp2((s - top) * e).astype(jnp.bfloat16))
                    keeps.append(jnp.exp2((old - top) * e))
                for u in range(group):
                    mix_e[side, first + u] = mix_e[side, first + u] * keeps[u] + dot(vt[first + u, :, keys], ps[u])

        lax.fori_loop(0, 4 * groups, pair, None)

        def done(side, _):
            for i in range(heads):
                weight = 1 / mix_e[side, i, HEAD : HEAD + 1, :]
                out = (mix_e[side, i, :HEAD, :] * weight).T.astype(ob.dtype)
                ob[pl.ds(pl.multiple_of(side * half, half), half), i * HEAD : (i + 1) * HEAD] = out

        lax.fori_loop(0, 2, done, None)

    def attend(i):
        def part(p, _):
            side, g = lax.div(p, groups), lax.rem(p, groups)
            at = place(i, side)
            here = pl.ds(at, half)
            first = g * group

            def head(u):
                return pl.ds(pl.multiple_of((first + u) * HEAD, HEAD), HEAD)

            for u in range(group):
                top_e[0, u] = jnp.full((1, half), NEG, jnp.float32)
                mix_e[0, u] = jnp.zeros((AUG, half), jnp.float32)

            def block(j, masked):
                keys = pl.ds(pl.multiple_of(j * KEYS, KEYS), KEYS)
                scores = [dot(kb[keys, head(u)], qb[here, head(u)], 1, 1) for u in range(group)]
                if masked:
                    gap = lax.broadcasted_iota(jnp.int32, (KEYS, half), 1) - lax.broadcasted_iota(jnp.int32, (KEYS, half), 0)
                    seen = gap >= j * KEYS - at
                tops, ps = [], []
                for u in range(group):
                    s = jnp.where(seen, scores[u], HIDDEN) if masked else scores[u]
                    old = top_e[0, u]
                    top = jnp.maximum(old, s.max(axis=0, keepdims=True))
                    top_e[0, u] = top
                    ps.append(jnp.exp2((s - top) * e).astype(jnp.bfloat16))
                    tops.append(jnp.exp2((old - top) * e))
                for u in range(group):
                    mix_e[0, u] = mix_e[0, u] * tops[u] + dot(vt[first + u, :, keys], ps[u])

            whole = lax.div(at, KEYS)
            lax.fori_loop(0, whole, lambda j, _: block(j, False), None)
            block(whole, True)
            for u in range(group):
                weight = 1 / mix_e[0, u, HEAD : HEAD + 1, :]
                ob[pl.ds(pl.multiple_of(side * half, half), half), head(u)] = (mix_e[0, u, :HEAD, :] * weight).T.astype(ob.dtype)

        lax.fori_loop(0, 2 * groups, part, None)

    def queries():
        others = [h for h in range(n) if h != 1]
        acc[...] = jnp.zeros_like(acc)

        def one(s, _):
            t = slices + s
            weights(t, 0).wait()
            for held, h in enumerate(others):
                acc[held] += dot(buf[h, s], wb[lax.rem(t, 2), 0])

            @pl.when(s + 2 < slices)
            def _():
                weights(t + 2, 0).start()

        lax.fori_loop(0, slices, one, None)
        for held, h in enumerate(others):
            turn(h, ((0, held),))

    def step(i, _):
        @pl.when(i == 1)
        def _():
            late()

        @pl.when(i == 2)
        def _():
            queries()
            sent(0)
            sent(2)
            for s in range(slices):
                x_slice(s).start()

        @pl.when(i > 1)
        def _():
            attend(i)

        k = n - 2 + i
        mine = k - (n - 2) * lax.div(1, i)

        def ship(c):
            @pl.when(i < n)
            def _():
                for way in range(2):
                    hop(way, k, c, mine).start()

        def chunk(c, _):
            t = (i - 1) * slices + c
            out_weights(t).wait()
            term[...] = dot(ob[...], wob[lax.rem(t, wos)])

            @pl.when(t + wos < total)
            def _():
                out_weights(t + wos).start()

            @pl.when(c > 0)
            def _():
                ship(c - 1)

            @pl.when(i > 1)
            def _():
                for way in range(2):
                    hop(way, k - 1, c).wait_recv()
                term[...] += buf[k, c].astype(jnp.float32)

            @pl.when(i < n)
            def _():
                buf[mine, c] = term[...].astype(buf.dtype)

            @pl.when(i == n)
            def _():
                x_slice(c).wait()
                buf[2, c] = (buf[0, c].astype(jnp.float32) + term[...]).astype(buf.dtype)

                @pl.when(c > 0)
                def _():
                    y_slice(c - 1).start()

        lax.fori_loop(0, slices, chunk, None)

        ship(slices - 1)

    lax.fori_loop(1, n + 1, step, None)
    y_slice(slices - 1).start()
    for k in range(n - 1, 2 * n - 2):
        sent(k)
    for s in range(slices):
        y_slice(s).wait()


def tables(tokens):
    half = HEAD // 2
    power = np.power(np.float32(THETA), -np.arange(half, dtype=np.float32) / np.float32(half)).astype(np.float32)
    angle = np.arange(tokens, dtype=np.float32)[:, None] * power
    return np.concatenate([np.cos(angle), np.sin(angle)], 1).astype(np.float32)


def solution(mesh):
    n = mesh.shape["tp"]

    def step(x, gain, wq, wk, wv, wo):
        rows, depth = x.shape
        columns = wq.shape[1]
        heads = columns // HEAD
        slices = depth // SLICE
        tokens = n * rows
        bf16, f32 = jnp.bfloat16, jnp.float32
        whole = pl.BlockSpec(memory_space=pltpu.VMEM)
        hbm = pl.BlockSpec(memory_space=pl.ANY)
        return pl.pallas_call(
            functools.partial(kernel, n, heads // 2),
            out_shape=jax.ShapeDtypeStruct((rows, depth), bf16),
            in_specs=[hbm, whole, whole, hbm, hbm, hbm, hbm],
            out_specs=hbm,
            scratch_shapes=[
                pltpu.VMEM((2 * n - 1, slices, rows, SLICE), bf16),
                pltpu.VMEM((2, 3, SLICE, columns), bf16),
                pltpu.VMEM((3, rows, columns), f32),
                pltpu.VMEM((tokens, columns), bf16),
                pltpu.VMEM((tokens, columns), bf16),
                pltpu.VMEM((heads, AUG, tokens), bf16),
                pltpu.VMEM((2, columns, SLICE), bf16),
                pltpu.VMEM((rows, columns), bf16),
                pltpu.VMEM((rows, SLICE), f32),
                pltpu.VMEM((2, heads, 1, rows // 2), f32),
                pltpu.VMEM((2, heads, AUG, rows // 2), f32),
                pltpu.SemaphoreType.DMA((2, 2 * n - 2, slices)),
                pltpu.SemaphoreType.DMA((2, 2 * n - 2, slices)),
                pltpu.SemaphoreType.DMA((2, 3)),
                pltpu.SemaphoreType.DMA((2,)),
                pltpu.SemaphoreType.DMA((slices,)),
            ],
            compiler_params=pltpu.CompilerParams(collective_id=0, has_side_effects=True, vmem_limit_bytes=67_000_000),
        )(x, gain.astype(f32).reshape(1, -1), tables(tokens), wq, wk, wv, wo)

    tokens, columns = P(("dp", "tp"), None), P(None, "tp")
    return jax.shard_map(
        step,
        mesh=mesh,
        in_specs=(tokens, P(None), columns, columns, columns, P("tp", None)),
        out_specs=tokens,
        check_vma=False,
    )
```

```python
import functools

import jax
import jax.numpy as jnp
import numpy as np
from jax import lax
from jax.experimental import pallas as pl
from jax.experimental.pallas import tpu as pltpu
from jax.sharding import PartitionSpec as P

HEAD = 128
THETA = 10000
SLICE = 512
KEYS = 256
NEG = -1e30
HIDDEN = 2 * NEG
LOG2E = 1.4426950408889634
MESH = pl.DeviceIdType.MESH
ORDER = (1, 2, 0)
AUG = HEAD + 16


def dot(a, b, ca=1, cb=0):
    return lax.dot_general(a, b, (((ca,), (cb,)), ((), ())), preferred_element_type=jnp.float32)


def kernel(n, group, x_ref, gain_ref, angle_ref, wq_ref, wk_ref, wv_ref, wo_ref, y_ref, buf, wb, acc, qb, kb, vt, wob, ob, term, top_e, mix_e,
           send_sem, recv_sem, w_sem, wo_sem, x_sem):
    me = lax.axis_index("tp")
    right, left = lax.rem(me + 1, n), lax.rem(me + n - 1, n)
    slices, rows = buf.shape[1], buf.shape[2]
    half = rows // 2
    depth = x_ref.shape[1]
    columns = wq_ref.shape[1]
    heads = columns // HEAD
    groups = heads // group
    wos = wob.shape[0]
    halves = (pl.ds(0, half), pl.ds(half, half))
    total = n * slices
    share = -(-heads // slices)
    e = HEAD**-0.5 * LOG2E

    def lanes(c, width=SLICE):
        return pl.ds(pl.multiple_of(c * width, width), width)

    def own(s):
        return y_ref.at[:, lanes(s)]

    def hop(way, k, s, source=None):
        source = y_ref.at[halves[way], lanes(s)] if isinstance(k, int) and k == 0 else buf.at[k - 1 if source is None else source, s, halves[way]]
        return pltpu.make_async_remote_copy(
            src_ref=source,
            dst_ref=buf.at[k, s, halves[way]],
            send_sem=send_sem.at[way, k, s],
            recv_sem=recv_sem.at[way, k, s],
            device_id={"tp": left if way else right},
            device_id_type=MESH,
        )

    def arrive(k, s):
        for way in range(2):
            hop(way, k, s, k).wait_recv()

    def weights(t, m):
        w = (wq_ref, wk_ref, wv_ref)[m]
        s, slot = lax.rem(t, slices), lax.rem(t, 2)
        return pltpu.make_async_copy(w.at[pl.ds(pl.multiple_of(s * SLICE, SLICE), SLICE)], wb.at[slot, m], w_sem.at[slot, m])

    def out_weights(t):
        slot = lax.rem(t, wos)
        return pltpu.make_async_copy(wo_ref.at[:, lanes(lax.rem(t, slices))], wob.at[slot], wo_sem.at[slot])

    def x_slice(s):
        return pltpu.make_async_copy(x_ref.at[:, lanes(s)], own(s), x_sem.at[s])

    def place(h, side):
        return pl.multiple_of((1 - side) * (lax.rem(me - h + n, n) * rows) + side * (lax.rem(me + h, n) * rows + half), half)

    barrier = pltpu.get_barrier_semaphore()
    for neighbour in (left, right):
        pl.semaphore_signal(barrier, inc=1, device_id={"tp": neighbour}, device_id_type=MESH)
    for s in range(slices):
        x_slice(s).start()
    acc[...] = jnp.zeros_like(acc)
    vt[:, HEAD:, :] = jnp.ones((heads, AUG - HEAD, vt.shape[2]), vt.dtype)

    def square(s, sums):
        x_slice(s).wait()
        wide = own(s)[...].astype(jnp.float32)
        wide = wide * wide
        for at in range(0, SLICE, 128):
            sums = sums + wide[:, at : at + 128]
        return sums

    sums = lax.fori_loop(0, slices, square, jnp.zeros((rows, 128), jnp.float32))
    for t in range(2):
        for m in ORDER:
            weights(t, m).start()
    scale = lax.rsqrt(jnp.sum(sums, axis=1, keepdims=True) * (1 / depth) + 1e-6)
    pl.semaphore_wait(barrier, 2)

    def norm(s, _):
        own(s)[...] = (own(s)[...].astype(jnp.float32) * scale * gain_ref[lanes(s)].astype(jnp.float32).reshape(1, SLICE)).astype(y_ref.dtype)

        @pl.when(s > 0)
        def _():
            for way in range(2):
                hop(way, 0, s - 1).start()

    lax.fori_loop(0, slices, norm, None)
    for way in range(2):
        hop(way, 0, slices - 1).start()

    def turn(h, parts):
        def side_of(side, _):
            mine = pl.ds(pl.multiple_of(side * half, half), half)
            here = pl.ds(place(h, side), half)
            both = angle_ref[here, :]
            other = pltpu.roll(both, HEAD // 2, axis=1)
            low = lax.broadcasted_iota(jnp.int32, both.shape, 1) < HEAD // 2
            cos, sin = jnp.where(low, both, other), jnp.where(low, -other, both)
            for i in range(heads):
                head = slice(i * HEAD, (i + 1) * HEAD)
                for m, held in parts:
                    if m == 2:
                        vt[i, :HEAD, here] = acc[held, mine, head].T.astype(vt.dtype)
                    else:
                        v = acc[held, mine, head].astype(jnp.bfloat16).astype(jnp.float32)
                        (qb, kb)[m][here, head] = (v * cos + pltpu.roll(v, HEAD // 2, axis=1) * sin).astype(kb.dtype)

        lax.fori_loop(0, 2, side_of, None)

    def product(block, t, m):
        weights(t, m).wait()
        acc[m] += dot(block[...], wb[lax.rem(t, 2), m])

    def keys_and_values(block, t):
        for m in (1, 2):
            product(block, t, m)

            @pl.when(t + 2 < total)
            def _():
                weights(t + 2, m).start()

    def turned(h):
        turn(h, ((1, 1), (2, 2)))
        acc[1:3] = jnp.zeros((2, *acc.shape[1:]), acc.dtype)

    def early(i):
        head = pl.ds(pl.multiple_of(i * HEAD, HEAD), HEAD)
        gap = lax.broadcasted_iota(jnp.int32, (half, half), 1) - lax.broadcasted_iota(jnp.int32, (half, half), 0)
        known = [place(h, side) for h in range(n - 1) for side in range(2)]
        all_scores = []
        for side in range(2):
            at = place(1, side)
            q = qb[pl.ds(at, half), head]
            all_scores.append([jnp.where(gap >= k - at, dot(kb[pl.ds(k, half), head], q, 1, 1), HIDDEN) for k in known])
        for side in range(2):
            scores = all_scores[side]
            top = functools.reduce(jnp.maximum, scores).max(axis=0, keepdims=True)
            top_e[side, i] = top
            mix_e[side, i] = sum(dot(vt[i, :, pl.ds(k, half)], jnp.exp2((s - top) * e).astype(jnp.bfloat16)) for k, s in zip(known, scores))

    def project(t, _):
        h, s = lax.div(t, slices), lax.rem(t, slices)

        @pl.when(h == n - 1)
        def _():
            for u in range(share):

                @pl.when(s * share + u < heads)
                def _():
                    early(s * share + u)

        arrive(h - 1, s)

        @pl.when(h < n - 1)
        def _():
            for way in range(2):
                hop(way, h, s).start()

        keys_and_values(buf.at[h - 1, s], t)

        @pl.when(h == 1)
        def _():
            product(buf.at[0, s], s, 0)
            weights(s + 2, 0).start()

        @pl.when((s == slices - 1) & (h < n - 1))
        def _():
            turned(h)

        @pl.when((s == slices - 1) & (h == 1))
        def _():
            turn(1, ((0, 0),))

    def sent(k):
        def one(s, _):
            for way in range(2):
                hop(way, k, s).wait_send()

        lax.fori_loop(0, slices, one, None)

    for t in range(wos):
        out_weights(t).start()
    lax.fori_loop(0, slices, lambda s, _: keys_and_values(own(s), s), None)
    turned(0)
    lax.fori_loop(slices, total, project, None)

    turn(n - 1, ((1, 1), (2, 2)))
    sent(1)

    def late():
        def pair(p, _):
            side, other, first = lax.div(p, 2 * groups), lax.rem(p, 2), lax.rem(lax.div(p, 2), groups) * group
            at, k = place(1, side), place(n - 1, other)
            here, keys = pl.ds(at, half), pl.ds(k, half)

            @pl.when(k < at)
            def _():
                heads_here = [pl.ds(pl.multiple_of((first + u) * HEAD, HEAD), HEAD) for u in range(group)]
                scores = [dot(kb[keys, head], qb[here, head], 1, 1) for head in heads_here]
                ps, keeps = [], []
                for u, s in enumerate(scores):
                    old = top_e[side, first + u]
                    top = jnp.maximum(old, s.max(axis=0, keepdims=True))
                    top_e[side, first + u] = top
                    ps.append(jnp.exp2((s - top) * e).astype(jnp.bfloat16))
                    keeps.append(jnp.exp2((old - top) * e))
                for u in range(group):
                    mix_e[side, first + u] = mix_e[side, first + u] * keeps[u] + dot(vt[first + u, :, keys], ps[u])

        lax.fori_loop(0, 4 * groups, pair, None)

        def done(side, _):
            for i in range(heads):
                weight = 1 / mix_e[side, i, HEAD : HEAD + 1, :]
                out = (mix_e[side, i, :HEAD, :] * weight).T.astype(ob.dtype)
                ob[pl.ds(pl.multiple_of(side * half, half), half), i * HEAD : (i + 1) * HEAD] = out

        lax.fori_loop(0, 2, done, None)

    def attend(i):
        def part(p, _):
            side, g = lax.div(p, groups), lax.rem(p, groups)
            at = place(i, side)
            here = pl.ds(at, half)
            first = g * group

            def head(u):
                return pl.ds(pl.multiple_of((first + u) * HEAD, HEAD), HEAD)

            for u in range(group):
                top_e[0, u] = jnp.full((1, half), NEG, jnp.float32)
                mix_e[0, u] = jnp.zeros((AUG, half), jnp.float32)

            def block(j, masked):
                keys = pl.ds(pl.multiple_of(j * KEYS, KEYS), KEYS)
                scores = [dot(kb[keys, head(u)], qb[here, head(u)], 1, 1) for u in range(group)]
                if masked:
                    gap = lax.broadcasted_iota(jnp.int32, (KEYS, half), 1) - lax.broadcasted_iota(jnp.int32, (KEYS, half), 0)
                    seen = gap >= j * KEYS - at
                tops, ps = [], []
                for u in range(group):
                    s = jnp.where(seen, scores[u], HIDDEN) if masked else scores[u]
                    old = top_e[0, u]
                    top = jnp.maximum(old, s.max(axis=0, keepdims=True))
                    top_e[0, u] = top
                    ps.append(jnp.exp2((s - top) * e).astype(jnp.bfloat16))
                    tops.append(jnp.exp2((old - top) * e))
                for u in range(group):
                    mix_e[0, u] = mix_e[0, u] * tops[u] + dot(vt[first + u, :, keys], ps[u])

            whole = lax.div(at, KEYS)
            lax.fori_loop(0, whole, lambda j, _: block(j, False), None)
            block(whole, True)
            for u in range(group):
                weight = 1 / mix_e[0, u, HEAD : HEAD + 1, :]
                ob[pl.ds(pl.multiple_of(side * half, half), half), head(u)] = (mix_e[0, u, :HEAD, :] * weight).T.astype(ob.dtype)

        lax.fori_loop(0, 2 * groups, part, None)

    def queries():
        others = [h for h in range(n) if h != 1]
        acc[...] = jnp.zeros_like(acc)

        def one(s, _):
            t = slices + s
            weights(t, 0).wait()
            for held, h in enumerate(others):
                acc[held] += dot(buf[h - 1, s] if h else own(s)[...], wb[lax.rem(t, 2), 0])

            @pl.when(s + 2 < slices)
            def _():
                weights(t + 2, 0).start()

        lax.fori_loop(0, slices, one, None)
        for held, h in enumerate(others):
            turn(h, ((0, held),))

    def step(i, _):
        @pl.when(i == 1)
        def _():
            late()

        @pl.when(i == 2)
        def _():
            queries()
            sent(0)
            for s in range(slices):
                x_slice(s).start()

        @pl.when(i > 1)
        def _():
            attend(i)

        k = n - 2 + i
        mine = k - 1 - (n - 2) * lax.div(1, i)

        def ship(c):
            @pl.when(i < n)
            def _():
                for way in range(2):
                    hop(way, k, c, mine).start()

        def chunk(c, _):
            t = (i - 1) * slices + c
            out_weights(t).wait()
            term[...] = dot(ob[...], wob[lax.rem(t, wos)])

            @pl.when(t + wos < total)
            def _():
                out_weights(t + wos).start()

            @pl.when(c > 0)
            def _():
                ship(c - 1)

            @pl.when(i > 1)
            def _():
                arrive(k - 1, c)
                term[...] += buf[k - 1, c].astype(jnp.float32)

            @pl.when(i < n)
            def _():
                buf[mine, c] = term[...].astype(buf.dtype)

            @pl.when(i == n)
            def _():
                x_slice(c).wait()
                own(c)[...] = (own(c)[...].astype(jnp.float32) + term[...]).astype(y_ref.dtype)

        lax.fori_loop(0, slices, chunk, None)

        ship(slices - 1)

    lax.fori_loop(1, n + 1, step, None)
    for k in range(2, 2 * n - 2):
        sent(k)


def tables(tokens):
    half = HEAD // 2
    power = np.power(np.float32(THETA), -np.arange(half, dtype=np.float32) / np.float32(half)).astype(np.float32)
    angle = np.arange(tokens, dtype=np.float32)[:, None] * power
    return np.concatenate([np.cos(angle), np.sin(angle)], 1).astype(np.float32)


def solution(mesh):
    n = mesh.shape["tp"]

    def step(x, gain, wq, wk, wv, wo):
        rows, depth = x.shape
        columns = wq.shape[1]
        heads = columns // HEAD
        slices = depth // SLICE
        tokens = n * rows
        bf16, f32 = jnp.bfloat16, jnp.float32
        whole = pl.BlockSpec(memory_space=pltpu.VMEM)
        hbm = pl.BlockSpec(memory_space=pl.ANY)
        return pl.pallas_call(
            functools.partial(kernel, n, heads // 2),
            out_shape=pltpu.VMEM((rows, depth), bf16),
            in_specs=[hbm, whole, whole, hbm, hbm, hbm, hbm],
            out_specs=whole,
            scratch_shapes=[
                pltpu.VMEM((2 * n - 2, slices, rows, SLICE), bf16),
                pltpu.VMEM((2, 3, SLICE, columns), bf16),
                pltpu.VMEM((3, rows, columns), f32),
                pltpu.VMEM((tokens, columns), bf16),
                pltpu.VMEM((tokens, columns), bf16),
                pltpu.VMEM((heads, AUG, tokens), bf16),
                pltpu.VMEM((2, columns, SLICE), bf16),
                pltpu.VMEM((rows, columns), bf16),
                pltpu.VMEM((rows, SLICE), f32),
                pltpu.VMEM((2, heads, 1, rows // 2), f32),
                pltpu.VMEM((2, heads, AUG, rows // 2), f32),
                pltpu.SemaphoreType.DMA((2, 2 * n - 2, slices)),
                pltpu.SemaphoreType.DMA((2, 2 * n - 2, slices)),
                pltpu.SemaphoreType.DMA((2, 3)),
                pltpu.SemaphoreType.DMA((2,)),
                pltpu.SemaphoreType.DMA((slices,)),
            ],
            compiler_params=pltpu.CompilerParams(collective_id=0, has_side_effects=True, vmem_limit_bytes=63_300_000),
        )(x, gain, tables(tokens), wq, wk, wv, wo)

    tokens, columns = P(("dp", "tp"), None), P(None, "tp")
    return jax.shard_map(
        step,
        mesh=mesh,
        in_specs=(tokens, P(None), columns, columns, columns, P("tp", None)),
        out_specs=tokens,
        check_vma=False,
    )
```

```python
import functools

import jax
import jax.numpy as jnp
import numpy as np
from jax import lax
from jax.experimental import pallas as pl
from jax.experimental.pallas import tpu as pltpu
from jax.sharding import PartitionSpec as P

HEAD = 128
THETA = 10000
SLICE = 512
KEYS = 256
NEG = -1e30
HIDDEN = 2 * NEG
LOG2E = 1.4426950408889634
MESH = pl.DeviceIdType.MESH
ORDER = (1, 2, 0)
AUG = HEAD + 16


def dot(a, b, ca=1, cb=0):
    return lax.dot_general(a, b, (((ca,), (cb,)), ((), ())), preferred_element_type=jnp.float32)


def kernel(n, group, x_ref, gain_ref, angle_ref, wq_ref, wk_ref, wv_ref, wo_ref, y_ref, buf, wb, acc, qb, kb, vt, wob, ob, term, top_e, mix_e,
           send_sem, recv_sem, w_sem, wo_sem, x_sem):
    me = lax.axis_index("tp")
    right, left = lax.rem(me + 1, n), lax.rem(me + n - 1, n)
    slices, rows = buf.shape[1], buf.shape[2]
    half = rows // 2
    depth = x_ref.shape[1]
    columns = wq_ref.shape[1]
    heads = columns // HEAD
    groups = heads // group
    wos = wob.shape[0]
    halves = (pl.ds(0, half), pl.ds(half, half))
    total = n * slices
    share = -(-heads // slices)
    e = HEAD**-0.5 * LOG2E

    def lanes(c, width=SLICE):
        return pl.ds(pl.multiple_of(c * width, width), width)

    def own(s):
        return y_ref.at[:, lanes(s)]

    def hop(way, k, s, source=None):
        source = y_ref.at[halves[way], lanes(s)] if isinstance(k, int) and k == 0 else buf.at[k - 1 if source is None else source, s, halves[way]]
        return pltpu.make_async_remote_copy(
            src_ref=source,
            dst_ref=buf.at[k, s, halves[way]],
            send_sem=send_sem.at[way, k, s],
            recv_sem=recv_sem.at[way, k, s],
            device_id={"tp": left if way else right},
            device_id_type=MESH,
        )

    def arrive(k, s):
        for way in range(2):
            hop(way, k, s, k).wait_recv()

    def weights(t, m):
        w = (wq_ref, wk_ref, wv_ref)[m]
        s, slot = lax.rem(t, slices), lax.rem(t, 2)
        return pltpu.make_async_copy(w.at[pl.ds(pl.multiple_of(s * SLICE, SLICE), SLICE)], wb.at[slot, m], w_sem.at[slot, m])

    def out_weights(t):
        slot = lax.rem(t, wos)
        return pltpu.make_async_copy(wo_ref.at[:, lanes(lax.rem(t, slices))], wob.at[slot], wo_sem.at[slot])

    def x_slice(s):
        return pltpu.make_async_copy(x_ref.at[:, lanes(s)], own(s), x_sem.at[s])

    def place(h, side):
        return pl.multiple_of((1 - side) * (lax.rem(me - h + n, n) * rows) + side * (lax.rem(me + h, n) * rows + half), half)

    barrier = pltpu.get_barrier_semaphore()
    for neighbour in (left, right):
        pl.semaphore_signal(barrier, inc=1, device_id={"tp": neighbour}, device_id_type=MESH)
    for s in range(slices):
        x_slice(s).start()
    acc[...] = jnp.zeros_like(acc)
    vt[:, HEAD:, :] = jnp.ones((heads, AUG - HEAD, vt.shape[2]), vt.dtype)

    def square(s, sums):
        x_slice(s).wait()
        wide = own(s)[...].astype(jnp.float32)
        wide = wide * wide
        for at in range(0, SLICE, 128):
            sums = sums + wide[:, at : at + 128]
        return sums

    sums = lax.fori_loop(0, slices, square, jnp.zeros((rows, 128), jnp.float32))
    for t in range(2):
        for m in ORDER:
            weights(t, m).start()
    scale = lax.rsqrt(jnp.sum(sums, axis=1, keepdims=True) * (1 / depth) + 1e-6)
    pl.semaphore_wait(barrier, 2)

    def norm(s, _):
        own(s)[...] = (own(s)[...].astype(jnp.float32) * scale * gain_ref[lanes(s)].astype(jnp.float32).reshape(1, SLICE)).astype(y_ref.dtype)

        @pl.when(s > 0)
        def _():
            for way in range(2):
                hop(way, 0, s - 1).start()

    lax.fori_loop(0, slices, norm, None)
    for way in range(2):
        hop(way, 0, slices - 1).start()

    def turn(h, parts):
        def side_of(side, _):
            mine = pl.ds(pl.multiple_of(side * half, half), half)
            here = pl.ds(place(h, side), half)
            both = angle_ref[here, :]
            other = pltpu.roll(both, HEAD // 2, axis=1)
            low = lax.broadcasted_iota(jnp.int32, both.shape, 1) < HEAD // 2
            cos, sin = jnp.where(low, both, other), jnp.where(low, -other, both)
            for i in range(heads):
                head = slice(i * HEAD, (i + 1) * HEAD)
                for m, held in parts:
                    if m == 2:
                        vt[i, :HEAD, here] = acc[held, mine, head].T.astype(vt.dtype)
                    else:
                        v = acc[held, mine, head].astype(jnp.bfloat16).astype(jnp.float32)
                        (qb, kb)[m][here, head] = (v * cos + pltpu.roll(v, HEAD // 2, axis=1) * sin).astype(kb.dtype)

        lax.fori_loop(0, 2, side_of, None)

    def product(block, t, m):
        weights(t, m).wait()
        acc[m] += dot(block[...], wb[lax.rem(t, 2), m])

    def keys_and_values(block, t):
        for m in (1, 2):
            product(block, t, m)

            @pl.when(t + 2 < total)
            def _():
                weights(t + 2, m).start()

    def turned(h):
        turn(h, ((1, 1), (2, 2)))
        acc[1:3] = jnp.zeros((2, *acc.shape[1:]), acc.dtype)

    def early(i):
        head = pl.ds(pl.multiple_of(i * HEAD, HEAD), HEAD)
        gap = lax.broadcasted_iota(jnp.int32, (half, half), 1) - lax.broadcasted_iota(jnp.int32, (half, half), 0)
        known = [place(h, side) for h in range(n - 1) for side in range(2)]
        all_scores = []
        for side in range(2):
            at = place(1, side)
            q = qb[pl.ds(at, half), head]
            all_scores.append([jnp.where(gap >= k - at, dot(kb[pl.ds(k, half), head], q, 1, 1), HIDDEN) for k in known])
        for side in range(2):
            scores = all_scores[side]
            top = functools.reduce(jnp.maximum, scores).max(axis=0, keepdims=True)
            top_e[side, i] = top
            mix_e[side, i] = sum(dot(vt[i, :, pl.ds(k, half)], jnp.exp2((s - top) * e).astype(jnp.bfloat16)) for k, s in zip(known, scores))

    def sent(k):
        def one(s, _):
            for way in range(2):
                hop(way, k, s).wait_send()

        lax.fori_loop(0, slices, one, None)

    def project(t, _):
        h, s = lax.div(t, slices), lax.rem(t, slices)

        @pl.when(h == n - 1)
        def _():
            for u in range(share):

                @pl.when(s * share + u < heads)
                def _():
                    early(s * share + u)

        arrive(h - 1, s)

        @pl.when(h < n - 1)
        def _():
            for way in range(2):
                hop(way, h, s).start()

        keys_and_values(buf.at[h - 1, s], t)

        @pl.when(h == 1)
        def _():
            product(buf.at[0, s], s, 0)
            weights(s + 2, 0).start()

        @pl.when((s == slices - 1) & (h < n - 1))
        def _():
            turned(h)

        @pl.when((s == slices - 1) & (h == n - 2))
        def _():
            sent(1)

        @pl.when((s == slices - 1) & (h == 1))
        def _():
            turn(1, ((0, 0),))

    for t in range(wos):
        out_weights(t).start()
    lax.fori_loop(0, slices, lambda s, _: keys_and_values(own(s), s), None)
    turned(0)
    lax.fori_loop(slices, total, project, None)

    turn(n - 1, ((1, 1), (2, 2)))

    def late():
        def pair(p, _):
            side, other, first = lax.div(p, 2 * groups), lax.rem(p, 2), lax.rem(lax.div(p, 2), groups) * group
            at, k = place(1, side), place(n - 1, other)
            here, keys = pl.ds(at, half), pl.ds(k, half)

            @pl.when(k < at)
            def _():
                heads_here = [pl.ds(pl.multiple_of((first + u) * HEAD, HEAD), HEAD) for u in range(group)]
                scores = [dot(kb[keys, head], qb[here, head], 1, 1) for head in heads_here]
                ps, keeps = [], []
                for u, s in enumerate(scores):
                    old = top_e[side, first + u]
                    top = jnp.maximum(old, s.max(axis=0, keepdims=True))
                    top_e[side, first + u] = top
                    ps.append(jnp.exp2((s - top) * e).astype(jnp.bfloat16))
                    keeps.append(jnp.exp2((old - top) * e))
                for u in range(group):
                    mix_e[side, first + u] = mix_e[side, first + u] * keeps[u] + dot(vt[first + u, :, keys], ps[u])

        lax.fori_loop(0, 4 * groups, pair, None)

        def done(side, _):
            for i in range(heads):
                weight = 1 / mix_e[side, i, HEAD : HEAD + 1, :]
                out = (mix_e[side, i, :HEAD, :] * weight).T.astype(ob.dtype)
                ob[pl.ds(pl.multiple_of(side * half, half), half), i * HEAD : (i + 1) * HEAD] = out

        lax.fori_loop(0, 2, done, None)

    def attend(i):
        def part(p, _):
            side, g = lax.div(p, groups), lax.rem(p, groups)
            at = place(i, side)
            here = pl.ds(at, half)
            first = g * group

            def head(u):
                return pl.ds(pl.multiple_of((first + u) * HEAD, HEAD), HEAD)

            for u in range(group):
                top_e[0, u] = jnp.full((1, half), NEG, jnp.float32)
                mix_e[0, u] = jnp.zeros((AUG, half), jnp.float32)

            def block(j, masked):
                keys = pl.ds(pl.multiple_of(j * KEYS, KEYS), KEYS)
                scores = [dot(kb[keys, head(u)], qb[here, head(u)], 1, 1) for u in range(group)]
                if masked:
                    gap = lax.broadcasted_iota(jnp.int32, (KEYS, half), 1) - lax.broadcasted_iota(jnp.int32, (KEYS, half), 0)
                    seen = gap >= j * KEYS - at
                tops, ps = [], []
                for u in range(group):
                    s = jnp.where(seen, scores[u], HIDDEN) if masked else scores[u]
                    old = top_e[0, u]
                    top = jnp.maximum(old, s.max(axis=0, keepdims=True))
                    top_e[0, u] = top
                    ps.append(jnp.exp2((s - top) * e).astype(jnp.bfloat16))
                    tops.append(jnp.exp2((old - top) * e))
                for u in range(group):
                    mix_e[0, u] = mix_e[0, u] * tops[u] + dot(vt[first + u, :, keys], ps[u])

            whole = lax.div(at, KEYS)
            lax.fori_loop(0, whole, lambda j, _: block(j, False), None)
            block(whole, True)
            for u in range(group):
                weight = 1 / mix_e[0, u, HEAD : HEAD + 1, :]
                ob[pl.ds(pl.multiple_of(side * half, half), half), head(u)] = (mix_e[0, u, :HEAD, :] * weight).T.astype(ob.dtype)

        lax.fori_loop(0, 2 * groups, part, None)

    def queries(hops, turn_of, last):
        acc[: len(hops)] = jnp.zeros((len(hops), *acc.shape[1:]), acc.dtype)

        def one(s, _):
            t = turn_of * slices + s
            weights(t, 0).wait()
            for held, h in enumerate(hops):
                acc[held] += dot(buf[h - 1, s] if h else own(s)[...], wb[lax.rem(t, 2), 0])

            @pl.when(t + 2 < (last + 1) * slices)
            def _():
                weights(t + 2, 0).start()

        lax.fori_loop(0, slices, one, None)
        for held, h in enumerate(hops):
            turn(h, ((0, held),))

    def step(i, _):
        @pl.when(i == 1)
        def _():
            late()

        @pl.when(i == 2)
        def _():
            queries((2,), 1, 2)

        @pl.when(i == 3)
        def _():
            queries((*range(3, n), 0), 2, 2)
            sent(0)
            for s in range(slices):
                x_slice(s).start()

        @pl.when(i > 1)
        def _():
            attend(i)

        k = n - 2 + i
        mine = k - 1 - (n - 2) * lax.div(1, i)

        def ship(c):
            @pl.when(i < n)
            def _():
                for way in range(2):
                    hop(way, k, c, mine).start()

        def chunk(c, _):
            t = (i - 1) * slices + c
            out_weights(t).wait()
            term[...] = dot(ob[...], wob[lax.rem(t, wos)])

            @pl.when(t + wos < total)
            def _():
                out_weights(t + wos).start()

            @pl.when(c > 0)
            def _():
                ship(c - 1)

            @pl.when(i > 1)
            def _():
                arrive(k - 1, c)
                term[...] += buf[k - 1, c].astype(jnp.float32)

            @pl.when(i < n)
            def _():
                buf[mine, c] = term[...].astype(buf.dtype)

            @pl.when(i == n)
            def _():
                x_slice(c).wait()
                own(c)[...] = (own(c)[...].astype(jnp.float32) + term[...]).astype(y_ref.dtype)

        lax.fori_loop(0, slices, chunk, None)

        ship(slices - 1)

    lax.fori_loop(1, n + 1, step, None)
    for k in range(2, 2 * n - 2):
        sent(k)


def tables(tokens):
    half = HEAD // 2
    power = np.power(np.float32(THETA), -np.arange(half, dtype=np.float32) / np.float32(half)).astype(np.float32)
    angle = np.arange(tokens, dtype=np.float32)[:, None] * power
    return np.concatenate([np.cos(angle), np.sin(angle)], 1).astype(np.float32)


def solution(mesh):
    n = mesh.shape["tp"]

    def step(x, gain, wq, wk, wv, wo):
        rows, depth = x.shape
        columns = wq.shape[1]
        heads = columns // HEAD
        slices = depth // SLICE
        tokens = n * rows
        bf16, f32 = jnp.bfloat16, jnp.float32
        whole = pl.BlockSpec(memory_space=pltpu.VMEM)
        hbm = pl.BlockSpec(memory_space=pl.ANY)
        return pl.pallas_call(
            functools.partial(kernel, n, heads // 2),
            out_shape=pltpu.VMEM((rows, depth), bf16),
            in_specs=[hbm, whole, whole, hbm, hbm, hbm, hbm],
            out_specs=whole,
            scratch_shapes=[
                pltpu.VMEM((2 * n - 2, slices, rows, SLICE), bf16),
                pltpu.VMEM((2, 3, SLICE, columns), bf16),
                pltpu.VMEM((3, rows, columns), f32),
                pltpu.VMEM((tokens, columns), bf16),
                pltpu.VMEM((tokens, columns), bf16),
                pltpu.VMEM((heads, AUG, tokens), bf16),
                pltpu.VMEM((2, columns, SLICE), bf16),
                pltpu.VMEM((rows, columns), bf16),
                pltpu.VMEM((rows, SLICE), f32),
                pltpu.VMEM((2, heads, 1, rows // 2), f32),
                pltpu.VMEM((2, heads, AUG, rows // 2), f32),
                pltpu.SemaphoreType.DMA((2, 2 * n - 2, slices)),
                pltpu.SemaphoreType.DMA((2, 2 * n - 2, slices)),
                pltpu.SemaphoreType.DMA((2, 3)),
                pltpu.SemaphoreType.DMA((2,)),
                pltpu.SemaphoreType.DMA((slices,)),
            ],
            compiler_params=pltpu.CompilerParams(collective_id=0, has_side_effects=True, vmem_limit_bytes=63_300_000),
        )(x, gain, tables(tokens), wq, wk, wv, wo)

    tokens, columns = P(("dp", "tp"), None), P(None, "tp")
    return jax.shard_map(
        step,
        mesh=mesh,
        in_specs=(tokens, P(None), columns, columns, columns, P("tp", None)),
        out_specs=tokens,
        check_vma=False,
    )
```

```python
import functools

import jax
import jax.numpy as jnp
import numpy as np
from jax import lax
from jax.experimental import pallas as pl
from jax.experimental.pallas import tpu as pltpu
from jax.sharding import PartitionSpec as P

HEAD = 128
THETA = 10000
SLICE = 512
KEYS = 256
NEG = -1e30
HIDDEN = 2 * NEG
LOG2E = 1.4426950408889634
MESH = pl.DeviceIdType.MESH
ORDER = (1, 2, 0)
AUG = HEAD + 16


def dot(a, b, ca=1, cb=0):
    return lax.dot_general(a, b, (((ca,), (cb,)), ((), ())), preferred_element_type=jnp.float32)


def kernel(n, group, x_ref, gain_hbm, angle_hbm, wq_ref, wk_ref, wv_ref, wo_ref, y_ref, gain_ref, angle_ref, buf, wb, acc, qb, kb, vt, wob, ob, term, top_e, mix_e,
           send_sem, recv_sem, w_sem, wo_sem, x_sem, small_sem):
    me = lax.axis_index("tp")
    right, left = lax.rem(me + 1, n), lax.rem(me + n - 1, n)
    slices, rows = buf.shape[1], buf.shape[2]
    half = rows // 2
    depth = x_ref.shape[1]
    columns = wq_ref.shape[1]
    heads = columns // HEAD
    groups = heads // group
    wos = wob.shape[0]
    halves = (pl.ds(0, half), pl.ds(half, half))
    total = n * slices
    share = -(-heads // slices)
    e = HEAD**-0.5 * LOG2E

    def lanes(c, width=SLICE):
        return pl.ds(pl.multiple_of(c * width, width), width)

    def own(s):
        return y_ref.at[:, lanes(s)]

    def hop(way, k, s, source=None):
        source = y_ref.at[halves[way], lanes(s)] if isinstance(k, int) and k == 0 else buf.at[k - 1 if source is None else source, s, halves[way]]
        return pltpu.make_async_remote_copy(
            src_ref=source,
            dst_ref=buf.at[k, s, halves[way]],
            send_sem=send_sem.at[way, k, s],
            recv_sem=recv_sem.at[way, k, s],
            device_id={"tp": left if way else right},
            device_id_type=MESH,
        )

    def arrive(k, s):
        for way in range(2):
            hop(way, k, s, k).wait_recv()

    def weights(t, m):
        w = (wq_ref, wk_ref, wv_ref)[m]
        s, slot = lax.rem(t, slices), lax.rem(t, 2)
        return pltpu.make_async_copy(w.at[pl.ds(pl.multiple_of(s * SLICE, SLICE), SLICE)], wb.at[slot, m], w_sem.at[slot, m])

    def out_weights(t):
        slot = lax.rem(t, wos)
        return pltpu.make_async_copy(wo_ref.at[:, lanes(lax.rem(t, slices))], wob.at[slot], wo_sem.at[slot])

    def x_slice(s):
        return pltpu.make_async_copy(x_ref.at[:, lanes(s)], own(s), x_sem.at[s])

    def place(h, side):
        return pl.multiple_of((1 - side) * (lax.rem(me - h + n, n) * rows) + side * (lax.rem(me + h, n) * rows + half), half)

    barrier = pltpu.get_barrier_semaphore()
    for neighbour in (left, right):
        pl.semaphore_signal(barrier, inc=1, device_id={"tp": neighbour}, device_id_type=MESH)
    for s in range(slices):
        x_slice(s).start()
    small = (pltpu.make_async_copy(gain_hbm, gain_ref, small_sem.at[0]), pltpu.make_async_copy(angle_hbm, angle_ref, small_sem.at[1]))
    for copy in small:
        copy.start()
    acc[...] = jnp.zeros_like(acc)
    vt[:, HEAD:, :] = jnp.ones((heads, AUG - HEAD, vt.shape[2]), vt.dtype)

    def square(s, sums):
        x_slice(s).wait()
        wide = own(s)[...].astype(jnp.float32)
        wide = wide * wide
        for at in range(0, SLICE, 128):
            sums = sums + wide[:, at : at + 128]
        return sums

    sums = lax.fori_loop(0, slices, square, jnp.zeros((rows, 128), jnp.float32))
    for t in range(2):
        for m in ORDER:
            weights(t, m).start()
    scale = lax.rsqrt(jnp.sum(sums, axis=1, keepdims=True) * (1 / depth) + 1e-6)
    for copy in small:
        copy.wait()
    pl.semaphore_wait(barrier, 2)

    def norm(s, _):
        own(s)[...] = (own(s)[...].astype(jnp.float32) * scale * gain_ref[lanes(s)].astype(jnp.float32).reshape(1, SLICE)).astype(y_ref.dtype)

        @pl.when(s > 0)
        def _():
            for way in range(2):
                hop(way, 0, s - 1).start()

    lax.fori_loop(0, slices, norm, None)
    for way in range(2):
        hop(way, 0, slices - 1).start()

    def turn(h, parts):
        def side_of(side, _):
            mine = pl.ds(pl.multiple_of(side * half, half), half)
            here = pl.ds(place(h, side), half)
            both = angle_ref[here, :]
            other = pltpu.roll(both, HEAD // 2, axis=1)
            low = lax.broadcasted_iota(jnp.int32, both.shape, 1) < HEAD // 2
            cos, sin = jnp.where(low, both, other), jnp.where(low, -other, both)
            for i in range(heads):
                head = slice(i * HEAD, (i + 1) * HEAD)
                for m, held in parts:
                    if m == 2:
                        vt[i, :HEAD, here] = acc[held, mine, head].T.astype(vt.dtype)
                    else:
                        v = acc[held, mine, head].astype(jnp.bfloat16).astype(jnp.float32)
                        (qb, kb)[m][here, head] = (v * cos + pltpu.roll(v, HEAD // 2, axis=1) * sin).astype(kb.dtype)

        lax.fori_loop(0, 2, side_of, None)

    def product(block, t, m):
        weights(t, m).wait()
        acc[m] += dot(block[...], wb[lax.rem(t, 2), m])

    def keys_and_values(block, t):
        for m in (1, 2):
            product(block, t, m)

            @pl.when(t + 2 < total)
            def _():
                weights(t + 2, m).start()

    def turned(h):
        turn(h, ((1, 1), (2, 2)))
        acc[1:3] = jnp.zeros((2, *acc.shape[1:]), acc.dtype)

    def early(i):
        head = pl.ds(pl.multiple_of(i * HEAD, HEAD), HEAD)
        gap = lax.broadcasted_iota(jnp.int32, (half, half), 1) - lax.broadcasted_iota(jnp.int32, (half, half), 0)
        known = [place(h, side) for h in range(n - 1) for side in range(2)]
        all_scores = []
        for side in range(2):
            at = place(1, side)
            q = qb[pl.ds(at, half), head]
            all_scores.append([jnp.where(gap >= k - at, dot(kb[pl.ds(k, half), head], q, 1, 1), HIDDEN) for k in known])
        for side in range(2):
            scores = all_scores[side]
            top = functools.reduce(jnp.maximum, scores).max(axis=0, keepdims=True)
            top_e[side, i] = top
            mix_e[side, i] = sum(dot(vt[i, :, pl.ds(k, half)], jnp.exp2((s - top) * e).astype(jnp.bfloat16)) for k, s in zip(known, scores))

    def sent(k):
        def one(s, _):
            for way in range(2):
                hop(way, k, s).wait_send()

        lax.fori_loop(0, slices, one, None)

    def project(t, _):
        h, s = lax.div(t, slices), lax.rem(t, slices)

        @pl.when(h == n - 1)
        def _():
            for u in range(share):

                @pl.when(s * share + u < heads)
                def _():
                    early(s * share + u)

        arrive(h - 1, s)

        @pl.when(h < n - 1)
        def _():
            for way in range(2):
                hop(way, h, s).start()

        keys_and_values(buf.at[h - 1, s], t)

        @pl.when(h == 1)
        def _():
            product(buf.at[0, s], s, 0)
            weights(s + 2, 0).start()

        @pl.when((s == slices - 1) & (h < n - 1))
        def _():
            turned(h)

        @pl.when((s == slices - 1) & (h == n - 2))
        def _():
            sent(1)

        @pl.when((s == slices - 1) & (h == 1))
        def _():
            turn(1, ((0, 0),))

    for t in range(wos):
        out_weights(t).start()
    lax.fori_loop(0, slices, lambda s, _: keys_and_values(own(s), s), None)
    turned(0)
    lax.fori_loop(slices, total, project, None)

    turn(n - 1, ((1, 1), (2, 2)))

    def late():
        def pair(p, _):
            side, other, first = lax.div(p, 2 * groups), lax.rem(p, 2), lax.rem(lax.div(p, 2), groups) * group
            at, k = place(1, side), place(n - 1, other)
            here, keys = pl.ds(at, half), pl.ds(k, half)

            @pl.when(k < at)
            def _():
                heads_here = [pl.ds(pl.multiple_of((first + u) * HEAD, HEAD), HEAD) for u in range(group)]
                scores = [dot(kb[keys, head], qb[here, head], 1, 1) for head in heads_here]
                ps, keeps = [], []
                for u, s in enumerate(scores):
                    old = top_e[side, first + u]
                    top = jnp.maximum(old, s.max(axis=0, keepdims=True))
                    top_e[side, first + u] = top
                    ps.append(jnp.exp2((s - top) * e).astype(jnp.bfloat16))
                    keeps.append(jnp.exp2((old - top) * e))
                for u in range(group):
                    mix_e[side, first + u] = mix_e[side, first + u] * keeps[u] + dot(vt[first + u, :, keys], ps[u])

        lax.fori_loop(0, 4 * groups, pair, None)

        def done(side, _):
            for i in range(heads):
                weight = 1 / mix_e[side, i, HEAD : HEAD + 1, :]
                out = (mix_e[side, i, :HEAD, :] * weight).T.astype(ob.dtype)
                ob[pl.ds(pl.multiple_of(side * half, half), half), i * HEAD : (i + 1) * HEAD] = out

        lax.fori_loop(0, 2, done, None)

    def attend(i):
        def part(p, _):
            side, g = lax.div(p, groups), lax.rem(p, groups)
            at = place(i, side)
            here = pl.ds(at, half)
            first = g * group

            def head(u):
                return pl.ds(pl.multiple_of((first + u) * HEAD, HEAD), HEAD)

            for u in range(group):
                top_e[0, u] = jnp.full((1, half), NEG, jnp.float32)
                mix_e[0, u] = jnp.zeros((AUG, half), jnp.float32)

            def block(j, masked):
                keys = pl.ds(pl.multiple_of(j * KEYS, KEYS), KEYS)
                scores = [dot(kb[keys, head(u)], qb[here, head(u)], 1, 1) for u in range(group)]
                if masked:
                    gap = lax.broadcasted_iota(jnp.int32, (KEYS, half), 1) - lax.broadcasted_iota(jnp.int32, (KEYS, half), 0)
                    seen = gap >= j * KEYS - at
                tops, ps = [], []
                for u in range(group):
                    s = jnp.where(seen, scores[u], HIDDEN) if masked else scores[u]
                    old = top_e[0, u]
                    top = jnp.maximum(old, s.max(axis=0, keepdims=True))
                    top_e[0, u] = top
                    ps.append(jnp.exp2((s - top) * e).astype(jnp.bfloat16))
                    tops.append(jnp.exp2((old - top) * e))
                for u in range(group):
                    mix_e[0, u] = mix_e[0, u] * tops[u] + dot(vt[first + u, :, keys], ps[u])

            whole = lax.div(at, KEYS)
            lax.fori_loop(0, whole, lambda j, _: block(j, False), None)
            block(whole, True)
            for u in range(group):
                weight = 1 / mix_e[0, u, HEAD : HEAD + 1, :]
                ob[pl.ds(pl.multiple_of(side * half, half), half), head(u)] = (mix_e[0, u, :HEAD, :] * weight).T.astype(ob.dtype)

        lax.fori_loop(0, 2 * groups, part, None)

    def queries(hops, turn_of, last):
        acc[: len(hops)] = jnp.zeros((len(hops), *acc.shape[1:]), acc.dtype)

        def one(s, _):
            t = turn_of * slices + s
            weights(t, 0).wait()
            for held, h in enumerate(hops):
                acc[held] += dot(buf[h - 1, s] if h else own(s)[...], wb[lax.rem(t, 2), 0])

            @pl.when(t + 2 < (last + 1) * slices)
            def _():
                weights(t + 2, 0).start()

        lax.fori_loop(0, slices, one, None)
        for held, h in enumerate(hops):
            turn(h, ((0, held),))

    def step(i, _):
        @pl.when(i == 1)
        def _():
            late()

        @pl.when(i == 2)
        def _():
            queries((2,), 1, 2)

        @pl.when(i == 3)
        def _():
            queries((*range(3, n), 0), 2, 2)
            sent(0)
            for s in range(slices):
                x_slice(s).start()

        @pl.when(i > 1)
        def _():
            attend(i)

        @pl.when(i == n)
        def _():
            for k in range(2, 2 * n - 3):
                sent(k)

        k = n - 2 + i
        mine = k - 1 - (n - 2) * lax.div(1, i)

        def ship(c):
            @pl.when(i < n)
            def _():
                for way in range(2):
                    hop(way, k, c, mine).start()

        def chunk(c, _):
            t = (i - 1) * slices + c
            out_weights(t).wait()
            term[...] = dot(ob[...], wob[lax.rem(t, wos)])

            @pl.when(t + wos < total)
            def _():
                out_weights(t + wos).start()

            @pl.when(c > 0)
            def _():
                ship(c - 1)

            @pl.when(i > 1)
            def _():
                arrive(k - 1, c)
                term[...] += buf[k - 1, c].astype(jnp.float32)

            @pl.when(i < n)
            def _():
                buf[mine, c] = term[...].astype(buf.dtype)

            @pl.when(i == n)
            def _():
                x_slice(c).wait()
                own(c)[...] = (own(c)[...].astype(jnp.float32) + term[...]).astype(y_ref.dtype)
                for way in range(2):
                    hop(way, 2 * n - 3, c).wait_send()

        lax.fori_loop(0, slices, chunk, None)

        ship(slices - 1)

    lax.fori_loop(1, n + 1, step, None)


def tables(tokens):
    half = HEAD // 2
    power = np.power(np.float32(THETA), -np.arange(half, dtype=np.float32) / np.float32(half)).astype(np.float32)
    angle = np.arange(tokens, dtype=np.float32)[:, None] * power
    return np.concatenate([np.cos(angle), np.sin(angle)], 1).astype(np.float32)


def solution(mesh):
    n = mesh.shape["tp"]

    def step(x, gain, wq, wk, wv, wo):
        rows, depth = x.shape
        columns = wq.shape[1]
        heads = columns // HEAD
        slices = depth // SLICE
        tokens = n * rows
        bf16, f32 = jnp.bfloat16, jnp.float32
        whole = pl.BlockSpec(memory_space=pltpu.VMEM)
        hbm = pl.BlockSpec(memory_space=pl.ANY)
        return pl.pallas_call(
            functools.partial(kernel, n, heads // 2),
            out_shape=pltpu.VMEM((rows, depth), bf16),
            in_specs=[hbm, hbm, hbm, hbm, hbm, hbm, hbm],
            out_specs=whole,
            scratch_shapes=[
                pltpu.VMEM((depth,), bf16),
                pltpu.VMEM((tokens, HEAD), f32),
                pltpu.VMEM((2 * n - 2, slices, rows, SLICE), bf16),
                pltpu.VMEM((2, 3, SLICE, columns), bf16),
                pltpu.VMEM((3, rows, columns), f32),
                pltpu.VMEM((tokens, columns), bf16),
                pltpu.VMEM((tokens, columns), bf16),
                pltpu.VMEM((heads, AUG, tokens), bf16),
                pltpu.VMEM((2, columns, SLICE), bf16),
                pltpu.VMEM((rows, columns), bf16),
                pltpu.VMEM((rows, SLICE), f32),
                pltpu.VMEM((2, heads, 1, rows // 2), f32),
                pltpu.VMEM((2, heads, AUG, rows // 2), f32),
                pltpu.SemaphoreType.DMA((2, 2 * n - 2, slices)),
                pltpu.SemaphoreType.DMA((2, 2 * n - 2, slices)),
                pltpu.SemaphoreType.DMA((2, 3)),
                pltpu.SemaphoreType.DMA((2,)),
                pltpu.SemaphoreType.DMA((slices,)),
                pltpu.SemaphoreType.DMA((2,)),
            ],
            compiler_params=pltpu.CompilerParams(collective_id=0, has_side_effects=True, vmem_limit_bytes=63_300_000),
        )(x, gain, tables(tokens), wq, wk, wv, wo)

    tokens, columns = P(("dp", "tp"), None), P(None, "tp")
    return jax.shard_map(
        step,
        mesh=mesh,
        in_specs=(tokens, P(None), columns, columns, columns, P("tp", None)),
        out_specs=tokens,
        check_vma=False,
    )
```

```python
import functools

import jax
import jax.numpy as jnp
import numpy as np
from jax import lax
from jax.experimental import pallas as pl
from jax.experimental.pallas import tpu as pltpu
from jax.sharding import PartitionSpec as P

HEAD = 128
THETA = 10000
SLICE = 512
KEYS = 256
NEG = -1e30
HIDDEN = 2 * NEG
LOG2E = 1.4426950408889634
MESH = pl.DeviceIdType.MESH
ORDER = (1, 2, 0)
AUG = HEAD + 16


def dot(a, b, ca=1, cb=0):
    return lax.dot_general(a, b, (((ca,), (cb,)), ((), ())), preferred_element_type=jnp.float32)


def kernel(n, group, x_ref, gain_hbm, angle_hbm, wq_ref, wk_ref, wv_ref, wo_ref, y_ref, gain_ref, angle_ref, buf, wb, acc, qb, kb, vt, wob, ob, term, top_e, mix_e,
           send_sem, recv_sem, w_sem, wo_sem, x_sem, small_sem):
    me = lax.axis_index("tp")
    right, left = lax.rem(me + 1, n), lax.rem(me + n - 1, n)
    slices, rows = buf.shape[1], buf.shape[2]
    half = rows // 2
    depth = x_ref.shape[1]
    columns = wq_ref.shape[1]
    heads = columns // HEAD
    groups = heads // group
    wos = wob.shape[0]
    halves = (pl.ds(0, half), pl.ds(half, half))
    total = n * slices
    share = -(-heads // slices)
    e = HEAD**-0.5 * LOG2E

    def lanes(c, width=SLICE):
        return pl.ds(pl.multiple_of(c * width, width), width)

    def own(s):
        return y_ref.at[:, lanes(s)]

    def hop(way, k, s, source=None):
        source = y_ref.at[halves[way], lanes(s)] if isinstance(k, int) and k == 0 else buf.at[k - 1 if source is None else source, s, halves[way]]
        return pltpu.make_async_remote_copy(
            src_ref=source,
            dst_ref=buf.at[k, s, halves[way]],
            send_sem=send_sem.at[way, k, s],
            recv_sem=recv_sem.at[way, k, s],
            device_id={"tp": left if way else right},
            device_id_type=MESH,
        )

    def arrive(k, s):
        for way in range(2):
            hop(way, k, s, k).wait_recv()

    def weights(t, m):
        w = (wq_ref, wk_ref, wv_ref)[m]
        s, slot = lax.rem(t, slices), lax.rem(t, 2)
        return pltpu.make_async_copy(w.at[pl.ds(pl.multiple_of(s * SLICE, SLICE), SLICE)], wb.at[slot, m], w_sem.at[slot, m])

    def out_weights(t):
        slot = lax.rem(t, wos)
        return pltpu.make_async_copy(wo_ref.at[:, lanes(lax.rem(t, slices))], wob.at[slot], wo_sem.at[slot])

    def x_slice(s):
        return pltpu.make_async_copy(x_ref.at[:, lanes(s)], own(s), x_sem.at[s])

    def place(h, side):
        return pl.multiple_of((1 - side) * (lax.rem(me - h + n, n) * rows) + side * (lax.rem(me + h, n) * rows + half), half)

    barrier = pltpu.get_barrier_semaphore()
    for neighbour in (left, right):
        pl.semaphore_signal(barrier, inc=1, device_id={"tp": neighbour}, device_id_type=MESH)
    for s in range(slices):
        x_slice(s).start()
    small = (pltpu.make_async_copy(gain_hbm, gain_ref, small_sem.at[0]), pltpu.make_async_copy(angle_hbm, angle_ref, small_sem.at[1]))
    for copy in small:
        copy.start()
    acc[...] = jnp.zeros_like(acc)
    vt[:, HEAD:, :] = jnp.ones((heads, AUG - HEAD, vt.shape[2]), vt.dtype)

    def square(s, sums):
        x_slice(s).wait()
        wide = own(s)[...].astype(jnp.float32)
        wide = wide * wide
        for at in range(0, SLICE, 128):
            sums = sums + wide[:, at : at + 128]
        return sums

    sums = lax.fori_loop(0, slices, square, jnp.zeros((rows, 128), jnp.float32))
    for t in range(2):
        for m in ORDER:
            weights(t, m).start()
    scale = lax.rsqrt(jnp.sum(sums, axis=1, keepdims=True) * (1 / depth) + 1e-6)
    for copy in small:
        copy.wait()
    pl.semaphore_wait(barrier, 2)

    def norm(s, _):
        own(s)[...] = (own(s)[...].astype(jnp.float32) * scale * gain_ref[lanes(s)].astype(jnp.float32).reshape(1, SLICE)).astype(y_ref.dtype)

        @pl.when(s > 0)
        def _():
            for way in range(2):
                hop(way, 0, s - 1).start()

    lax.fori_loop(0, slices, norm, None)
    for way in range(2):
        hop(way, 0, slices - 1).start()

    def turn(h, parts):
        def side_of(side, _):
            mine = pl.ds(pl.multiple_of(side * half, half), half)
            here = pl.ds(place(h, side), half)
            both = angle_ref[here, :]
            other = pltpu.roll(both, HEAD // 2, axis=1)
            low = lax.broadcasted_iota(jnp.int32, both.shape, 1) < HEAD // 2
            cos, sin = jnp.where(low, both, other), jnp.where(low, -other, both)
            for i in range(heads):
                head = slice(i * HEAD, (i + 1) * HEAD)
                for m, held in parts:
                    if m == 2:
                        vt[i, :HEAD, here] = acc[held, mine, head].astype(vt.dtype).T
                    else:
                        v = acc[held, mine, head].astype(jnp.bfloat16)
                        swapped = pltpu.roll(v, HEAD // 2, axis=1).astype(jnp.float32)
                        (qb, kb)[m][here, head] = (v.astype(jnp.float32) * cos + swapped * sin).astype(kb.dtype)

        lax.fori_loop(0, 2, side_of, None)

    def product(block, t, m):
        weights(t, m).wait()
        acc[m] += dot(block[...], wb[lax.rem(t, 2), m])

    def keys_and_values(block, t):
        for m in (1, 2):
            product(block, t, m)

            @pl.when(t + 2 < total)
            def _():
                weights(t + 2, m).start()

    def turned(h):
        turn(h, ((1, 1), (2, 2)))
        acc[1:3] = jnp.zeros((2, *acc.shape[1:]), acc.dtype)

    def early(i):
        head = pl.ds(pl.multiple_of(i * HEAD, HEAD), HEAD)
        gap = lax.broadcasted_iota(jnp.int32, (half, half), 1) - lax.broadcasted_iota(jnp.int32, (half, half), 0)
        known = [place(h, side) for h in range(n - 1) for side in range(2)]
        all_scores = []
        for side in range(2):
            at = place(1, side)
            q = qb[pl.ds(at, half), head]
            all_scores.append([jnp.where(gap >= k - at, dot(kb[pl.ds(k, half), head], q, 1, 1), HIDDEN) for k in known])
        for side in range(2):
            scores = all_scores[side]
            top = functools.reduce(jnp.maximum, scores).max(axis=0, keepdims=True)
            top_e[side, i] = top
            mix_e[side, i] = sum(dot(vt[i, :, pl.ds(k, half)], jnp.exp2((s - top) * e).astype(jnp.bfloat16)) for k, s in zip(known, scores))

    def sent(k):
        def one(s, _):
            for way in range(2):
                hop(way, k, s).wait_send()

        lax.fori_loop(0, slices, one, None)

    def project(t, _):
        h, s = lax.div(t, slices), lax.rem(t, slices)

        @pl.when(h == n - 1)
        def _():
            for u in range(share):

                @pl.when(s * share + u < heads)
                def _():
                    early(s * share + u)

        arrive(h - 1, s)

        @pl.when(h < n - 1)
        def _():
            for way in range(2):
                hop(way, h, s).start()

        keys_and_values(buf.at[h - 1, s], t)

        @pl.when(h == 1)
        def _():
            product(buf.at[0, s], s, 0)
            weights(s + 2, 0).start()

        @pl.when((s == slices - 1) & (h < n - 1))
        def _():
            turned(h)

        @pl.when((s == slices - 1) & (h == n - 2))
        def _():
            sent(1)

        @pl.when((s == slices - 1) & (h == 1))
        def _():
            turn(1, ((0, 0),))

    for t in range(wos):
        out_weights(t).start()
    lax.fori_loop(0, slices, lambda s, _: keys_and_values(own(s), s), None)
    turned(0)
    lax.fori_loop(slices, total, project, None)

    turn(n - 1, ((1, 1), (2, 2)))

    def late():
        def pair(p, _):
            side, other = lax.div(p, 2), lax.rem(p, 2)
            at, k = place(1, side), place(n - 1, other)
            here, keys = pl.ds(at, half), pl.ds(k, half)

            @pl.when(k < at)
            def _():
                scores = [dot(kb[keys, i * HEAD : (i + 1) * HEAD], qb[here, i * HEAD : (i + 1) * HEAD], 1, 1) for i in range(heads)]
                ps, keeps = [], []
                for i, s in enumerate(scores):
                    old = top_e[side, i]
                    top = jnp.maximum(old, s.max(axis=0, keepdims=True))
                    top_e[side, i] = top
                    ps.append(jnp.exp2((s - top) * e).astype(jnp.bfloat16))
                    keeps.append(jnp.exp2((old - top) * e))
                for i in range(heads):
                    mix_e[side, i] = mix_e[side, i] * keeps[i] + dot(vt[i, :, keys], ps[i])

        lax.fori_loop(0, 4, pair, None)

        def done(side, _):
            for i in range(heads):
                weight = 1 / mix_e[side, i, HEAD : HEAD + 1, :]
                out = (mix_e[side, i, :HEAD, :] * weight).astype(ob.dtype).T
                ob[pl.ds(pl.multiple_of(side * half, half), half), i * HEAD : (i + 1) * HEAD] = out

        lax.fori_loop(0, 2, done, None)

    def attend(i):
        def part(p, _):
            side, g = lax.div(p, groups), lax.rem(p, groups)
            at = place(i, side)
            here = pl.ds(at, half)
            first = g * group

            def head(u):
                return pl.ds(pl.multiple_of((first + u) * HEAD, HEAD), HEAD)

            for u in range(group):
                top_e[0, u] = jnp.full((1, half), NEG, jnp.float32)
                mix_e[0, u] = jnp.zeros((AUG, half), jnp.float32)

            def block(j, masked):
                keys = pl.ds(pl.multiple_of(j * KEYS, KEYS), KEYS)
                scores = [dot(kb[keys, head(u)], qb[here, head(u)], 1, 1) for u in range(group)]
                if masked:
                    gap = lax.broadcasted_iota(jnp.int32, (KEYS, half), 1) - lax.broadcasted_iota(jnp.int32, (KEYS, half), 0)
                    seen = gap >= j * KEYS - at
                tops, ps = [], []
                for u in range(group):
                    s = jnp.where(seen, scores[u], HIDDEN) if masked else scores[u]
                    old = top_e[0, u]
                    top = jnp.maximum(old, s.max(axis=0, keepdims=True))
                    top_e[0, u] = top
                    ps.append(jnp.exp2((s - top) * e).astype(jnp.bfloat16))
                    tops.append(jnp.exp2((old - top) * e))
                for u in range(group):
                    mix_e[0, u] = mix_e[0, u] * tops[u] + dot(vt[first + u, :, keys], ps[u])

            whole = lax.div(at, KEYS)
            lax.fori_loop(0, whole, lambda j, _: block(j, False), None)
            block(whole, True)
            for u in range(group):
                weight = 1 / mix_e[0, u, HEAD : HEAD + 1, :]
                ob[pl.ds(pl.multiple_of(side * half, half), half), head(u)] = (mix_e[0, u, :HEAD, :] * weight).astype(ob.dtype).T

        lax.fori_loop(0, 2 * groups, part, None)

    def queries(hops, turn_of, last):
        acc[: len(hops)] = jnp.zeros((len(hops), *acc.shape[1:]), acc.dtype)

        def one(s, _):
            t = turn_of * slices + s
            weights(t, 0).wait()
            for held, h in enumerate(hops):
                acc[held] += dot(buf[h - 1, s] if h else own(s)[...], wb[lax.rem(t, 2), 0])

            @pl.when(t + 2 < (last + 1) * slices)
            def _():
                weights(t + 2, 0).start()

        lax.fori_loop(0, slices, one, None)
        for held, h in enumerate(hops):
            turn(h, ((0, held),))

    def step(i, _):
        @pl.when(i == 1)
        def _():
            late()

        @pl.when(i == 2)
        def _():
            queries((2,), 1, 2)

        @pl.when(i == 3)
        def _():
            queries((*range(3, n), 0), 2, 2)
            sent(0)
            for s in range(slices):
                x_slice(s).start()

        @pl.when(i > 1)
        def _():
            attend(i)

        @pl.when(i == n)
        def _():
            for k in range(2, 2 * n - 3):
                sent(k)

        k = n - 2 + i
        mine = k - 1 - (n - 2) * lax.div(1, i)

        def ship(c):
            @pl.when(i < n)
            def _():
                for way in range(2):
                    hop(way, k, c, mine).start()

        def chunk(c, _):
            t = (i - 1) * slices + c
            out_weights(t).wait()
            term[...] = dot(ob[...], wob[lax.rem(t, wos)])

            @pl.when(t + wos < total)
            def _():
                out_weights(t + wos).start()

            @pl.when(c > 0)
            def _():
                ship(c - 1)

            @pl.when(i > 1)
            def _():
                arrive(k - 1, c)
                term[...] += buf[k - 1, c].astype(jnp.float32)

            @pl.when(i < n)
            def _():
                buf[mine, c] = term[...].astype(buf.dtype)

            @pl.when(i == n)
            def _():
                x_slice(c).wait()
                own(c)[...] = (own(c)[...].astype(jnp.float32) + term[...]).astype(y_ref.dtype)
                for way in range(2):
                    hop(way, 2 * n - 3, c).wait_send()

        lax.fori_loop(0, slices, chunk, None)

        ship(slices - 1)

    lax.fori_loop(1, n + 1, step, None)


def tables(tokens):
    half = HEAD // 2
    power = np.power(np.float32(THETA), -np.arange(half, dtype=np.float32) / np.float32(half)).astype(np.float32)
    angle = np.arange(tokens, dtype=np.float32)[:, None] * power
    return np.concatenate([np.cos(angle), np.sin(angle)], 1).astype(np.float32)


def solution(mesh):
    n = mesh.shape["tp"]

    def step(x, gain, wq, wk, wv, wo):
        rows, depth = x.shape
        columns = wq.shape[1]
        heads = columns // HEAD
        slices = depth // SLICE
        tokens = n * rows
        bf16, f32 = jnp.bfloat16, jnp.float32
        whole = pl.BlockSpec(memory_space=pltpu.VMEM)
        hbm = pl.BlockSpec(memory_space=pl.ANY)
        return pl.pallas_call(
            functools.partial(kernel, n, heads // 2),
            out_shape=pltpu.VMEM((rows, depth), bf16),
            in_specs=[hbm, hbm, hbm, hbm, hbm, hbm, hbm],
            out_specs=whole,
            scratch_shapes=[
                pltpu.VMEM((depth,), bf16),
                pltpu.VMEM((tokens, HEAD), f32),
                pltpu.VMEM((2 * n - 2, slices, rows, SLICE), bf16),
                pltpu.VMEM((2, 3, SLICE, columns), bf16),
                pltpu.VMEM((3, rows, columns), f32),
                pltpu.VMEM((tokens, columns), bf16),
                pltpu.VMEM((tokens, columns), bf16),
                pltpu.VMEM((heads, AUG, tokens), bf16),
                pltpu.VMEM((2, columns, SLICE), bf16),
                pltpu.VMEM((rows, columns), bf16),
                pltpu.VMEM((rows, SLICE), f32),
                pltpu.VMEM((2, heads, 1, rows // 2), f32),
                pltpu.VMEM((2, heads, AUG, rows // 2), f32),
                pltpu.SemaphoreType.DMA((2, 2 * n - 2, slices)),
                pltpu.SemaphoreType.DMA((2, 2 * n - 2, slices)),
                pltpu.SemaphoreType.DMA((2, 3)),
                pltpu.SemaphoreType.DMA((2,)),
                pltpu.SemaphoreType.DMA((slices,)),
                pltpu.SemaphoreType.DMA((2,)),
            ],
            compiler_params=pltpu.CompilerParams(collective_id=0, has_side_effects=True, vmem_limit_bytes=63_300_000),
        )(x, gain, tables(tokens), wq, wk, wv, wo)

    tokens, columns = P(("dp", "tp"), None), P(None, "tp")
    return jax.shard_map(
        step,
        mesh=mesh,
        in_specs=(tokens, P(None), columns, columns, columns, P("tp", None)),
        out_specs=tokens,
        check_vma=False,
    )
```

```python
import functools

import jax
import jax.numpy as jnp
import numpy as np
from jax import lax
from jax.experimental import pallas as pl
from jax.experimental.pallas import tpu as pltpu
from jax.sharding import PartitionSpec as P

HEAD = 128
THETA = 10000
SLICE = 512
KEYS = 256
NEG = -1e30
HIDDEN = 2 * NEG
LOG2E = 1.4426950408889634
MESH = pl.DeviceIdType.MESH
ORDER = (1, 2, 0)
AUG = HEAD + 16


def dot(a, b, ca=1, cb=0):
    return lax.dot_general(a, b, (((ca,), (cb,)), ((), ())), preferred_element_type=jnp.float32)


def kernel(n, group, x_ref, gain_hbm, angle_hbm, wq_ref, wk_ref, wv_ref, wo_ref, y_ref, gain_ref, angle_ref, buf, wb, acc, qb, kb, vt, wob, ob, term, top_e, mix_e,
           send_sem, recv_sem, w_sem, wo_sem, x_sem, small_sem):
    me = lax.axis_index("tp")
    right, left = lax.rem(me + 1, n), lax.rem(me + n - 1, n)
    slices, rows = buf.shape[1], buf.shape[2]
    half = rows // 2
    depth = x_ref.shape[1]
    columns = wq_ref.shape[1]
    heads = columns // HEAD
    groups = heads // group
    wos = wob.shape[0]
    halves = (pl.ds(0, half), pl.ds(half, half))
    total = n * slices
    share = -(-heads // slices)
    e = HEAD**-0.5 * LOG2E

    def lanes(c, width=SLICE):
        return pl.ds(pl.multiple_of(c * width, width), width)

    def own(s):
        return y_ref.at[:, lanes(s)]

    def hop(way, k, s, source=None):
        source = y_ref.at[halves[way], lanes(s)] if isinstance(k, int) and k == 0 else buf.at[k - 1 if source is None else source, s, halves[way]]
        return pltpu.make_async_remote_copy(
            src_ref=source,
            dst_ref=buf.at[k, s, halves[way]],
            send_sem=send_sem.at[way, k, s],
            recv_sem=recv_sem.at[way, k, s],
            device_id={"tp": left if way else right},
            device_id_type=MESH,
        )

    def arrive(k, s):
        for way in range(2):
            hop(way, k, s, k).wait_recv()

    def weights(t, m):
        w = (wq_ref, wk_ref, wv_ref)[m]
        s, slot = lax.rem(t, slices), lax.rem(t, 2)
        return pltpu.make_async_copy(w.at[pl.ds(pl.multiple_of(s * SLICE, SLICE), SLICE)], wb.at[slot, m], w_sem.at[slot, m])

    def query_weights(t):
        at = (lax.rem(t, 2), lax.rem(t, 3))
        s = lax.rem(t, slices)
        return pltpu.make_async_copy(wq_ref.at[pl.ds(pl.multiple_of(s * SLICE, SLICE), SLICE)], wb.at[at], w_sem.at[at])

    def out_weights(t):
        slot = lax.rem(t, wos)
        return pltpu.make_async_copy(wo_ref.at[:, lanes(lax.rem(t, slices))], wob.at[slot], wo_sem.at[slot])

    def x_slice(s):
        return pltpu.make_async_copy(x_ref.at[:, lanes(s)], own(s), x_sem.at[s])

    def place(h, side):
        return pl.multiple_of((1 - side) * (lax.rem(me - h + n, n) * rows) + side * (lax.rem(me + h, n) * rows + half), half)

    barrier = pltpu.get_barrier_semaphore()
    for neighbour in (left, right):
        pl.semaphore_signal(barrier, inc=1, device_id={"tp": neighbour}, device_id_type=MESH)
    for s in range(slices):
        x_slice(s).start()
    small = (pltpu.make_async_copy(gain_hbm, gain_ref, small_sem.at[0]), pltpu.make_async_copy(angle_hbm, angle_ref, small_sem.at[1]))
    for copy in small:
        copy.start()
    acc[...] = jnp.zeros_like(acc)
    vt[:, HEAD:, :] = jnp.ones((heads, AUG - HEAD, vt.shape[2]), vt.dtype)

    def square(s, sums):
        x_slice(s).wait()
        wide = own(s)[...].astype(jnp.float32)
        wide = wide * wide
        for at in range(0, SLICE, 128):
            sums = sums + wide[:, at : at + 128]
        return sums

    sums = lax.fori_loop(0, slices, square, jnp.zeros((rows, 128), jnp.float32))
    for t in range(2):
        for m in ORDER:
            weights(t, m).start()
    scale = lax.rsqrt(jnp.sum(sums, axis=1, keepdims=True) * (1 / depth) + 1e-6)
    for copy in small:
        copy.wait()
    pl.semaphore_wait(barrier, 2)

    def norm(s, _):
        own(s)[...] = (own(s)[...].astype(jnp.float32) * scale * gain_ref[lanes(s)].astype(jnp.float32).reshape(1, SLICE)).astype(y_ref.dtype)

        @pl.when(s > 0)
        def _():
            for way in range(2):
                hop(way, 0, s - 1).start()

    lax.fori_loop(0, slices, norm, None)
    for way in range(2):
        hop(way, 0, slices - 1).start()

    def turn(h, parts):
        def side_of(side, _):
            mine = pl.ds(pl.multiple_of(side * half, half), half)
            here = pl.ds(place(h, side), half)
            both = angle_ref[here, :]
            other = pltpu.roll(both, HEAD // 2, axis=1)
            low = lax.broadcasted_iota(jnp.int32, both.shape, 1) < HEAD // 2
            cos, sin = jnp.where(low, both, other), jnp.where(low, -other, both)
            for i in range(heads):
                head = slice(i * HEAD, (i + 1) * HEAD)
                for m, held in parts:
                    if m == 2:
                        vt[i, :HEAD, here] = acc[held, mine, head].astype(vt.dtype).T
                    else:
                        v = acc[held, mine, head].astype(jnp.bfloat16)
                        swapped = pltpu.roll(v, HEAD // 2, axis=1).astype(jnp.float32)
                        (qb, kb)[m][here, head] = (v.astype(jnp.float32) * cos + swapped * sin).astype(kb.dtype)

        lax.fori_loop(0, 2, side_of, None)

    def product(block, t, m):
        weights(t, m).wait()
        acc[m] += dot(block[...], wb[lax.rem(t, 2), m])

    def keys_and_values(block, t):
        for m in (1, 2):
            product(block, t, m)

            @pl.when(t + 2 < total)
            def _():
                weights(t + 2, m).start()

    def turned(h):
        turn(h, ((1, 1), (2, 2)))
        acc[1:3] = jnp.zeros((2, *acc.shape[1:]), acc.dtype)

    def early(i):
        head = pl.ds(pl.multiple_of(i * HEAD, HEAD), HEAD)
        gap = lax.broadcasted_iota(jnp.int32, (half, half), 1) - lax.broadcasted_iota(jnp.int32, (half, half), 0)
        known = [place(h, side) for h in range(n - 1) for side in range(2)]
        all_scores = []
        for side in range(2):
            at = place(1, side)
            q = qb[pl.ds(at, half), head]
            all_scores.append([jnp.where(gap >= k - at, dot(kb[pl.ds(k, half), head], q, 1, 1), HIDDEN) for k in known])
        for side in range(2):
            scores = all_scores[side]
            top = functools.reduce(jnp.maximum, scores).max(axis=0, keepdims=True)
            top_e[side, i] = top
            mix_e[side, i] = sum(dot(vt[i, :, pl.ds(k, half)], jnp.exp2((s - top) * e).astype(jnp.bfloat16)) for k, s in zip(known, scores))

    def sent(k):
        def one(s, _):
            for way in range(2):
                hop(way, k, s).wait_send()

        lax.fori_loop(0, slices, one, None)

    def project(t, _):
        h, s = lax.div(t, slices), lax.rem(t, slices)

        @pl.when(h == n - 1)
        def _():
            for u in range(share):

                @pl.when(s * share + u < heads)
                def _():
                    early(s * share + u)

        arrive(h - 1, s)

        @pl.when(h < n - 1)
        def _():
            for way in range(2):
                hop(way, h, s).start()

        keys_and_values(buf.at[h - 1, s], t)

        @pl.when(h == 1)
        def _():
            product(buf.at[0, s], s, 0)

            @pl.when(s + 2 < slices)
            def _():
                weights(s + 2, 0).start()

        @pl.when((s == slices - 1) & (h < n - 1))
        def _():
            turned(h)

        @pl.when((s == slices - 1) & (h == n - 2))
        def _():
            sent(1)

        @pl.when((s == slices - 1) & (h == 1))
        def _():
            turn(1, ((0, 0),))

    for t in range(wos):
        out_weights(t).start()
    lax.fori_loop(0, slices, lambda s, _: keys_and_values(own(s), s), None)
    turned(0)
    lax.fori_loop(slices, total, project, None)

    turn(n - 1, ((1, 1), (2, 2)))

    def late():
        def pair(p, _):
            side, other = lax.div(p, 2), lax.rem(p, 2)
            at, k = place(1, side), place(n - 1, other)
            here, keys = pl.ds(at, half), pl.ds(k, half)

            @pl.when(k < at)
            def _():
                scores = [dot(kb[keys, i * HEAD : (i + 1) * HEAD], qb[here, i * HEAD : (i + 1) * HEAD], 1, 1) for i in range(heads)]
                ps, keeps = [], []
                for i, s in enumerate(scores):
                    old = top_e[side, i]
                    top = jnp.maximum(old, s.max(axis=0, keepdims=True))
                    top_e[side, i] = top
                    ps.append(jnp.exp2((s - top) * e).astype(jnp.bfloat16))
                    keeps.append(jnp.exp2((old - top) * e))
                for i in range(heads):
                    mix_e[side, i] = mix_e[side, i] * keeps[i] + dot(vt[i, :, keys], ps[i])

        lax.fori_loop(0, 4, pair, None)

        def done(side, _):
            for i in range(heads):
                weight = 1 / mix_e[side, i, HEAD : HEAD + 1, :]
                out = (mix_e[side, i, :HEAD, :] * weight).astype(ob.dtype).T
                ob[pl.ds(pl.multiple_of(side * half, half), half), i * HEAD : (i + 1) * HEAD] = out

        lax.fori_loop(0, 2, done, None)

    def attend(i):
        def part(p, _):
            side, g = lax.div(p, groups), lax.rem(p, groups)
            at = place(i, side)
            here = pl.ds(at, half)
            first = g * group

            def head(u):
                return pl.ds(pl.multiple_of((first + u) * HEAD, HEAD), HEAD)

            for u in range(group):
                top_e[0, u] = jnp.full((1, half), NEG, jnp.float32)
                mix_e[0, u] = jnp.zeros((AUG, half), jnp.float32)

            def block(j, masked):
                keys = pl.ds(pl.multiple_of(j * KEYS, KEYS), KEYS)
                scores = [dot(kb[keys, head(u)], qb[here, head(u)], 1, 1) for u in range(group)]
                if masked:
                    gap = lax.broadcasted_iota(jnp.int32, (KEYS, half), 1) - lax.broadcasted_iota(jnp.int32, (KEYS, half), 0)
                    seen = gap >= j * KEYS - at
                tops, ps = [], []
                for u in range(group):
                    s = jnp.where(seen, scores[u], HIDDEN) if masked else scores[u]
                    old = top_e[0, u]
                    top = jnp.maximum(old, s.max(axis=0, keepdims=True))
                    top_e[0, u] = top
                    ps.append(jnp.exp2((s - top) * e).astype(jnp.bfloat16))
                    tops.append(jnp.exp2((old - top) * e))
                for u in range(group):
                    mix_e[0, u] = mix_e[0, u] * tops[u] + dot(vt[first + u, :, keys], ps[u])

            whole = lax.div(at, KEYS)
            lax.fori_loop(0, whole, lambda j, _: block(j, False), None)
            block(whole, True)
            for u in range(group):
                weight = 1 / mix_e[0, u, HEAD : HEAD + 1, :]
                ob[pl.ds(pl.multiple_of(side * half, half), half), head(u)] = (mix_e[0, u, :HEAD, :] * weight).astype(ob.dtype).T

        lax.fori_loop(0, 2 * groups, part, None)

    def queries(hops, turn_of, last):
        acc[: len(hops)] = jnp.zeros((len(hops), *acc.shape[1:]), acc.dtype)

        def one(s, _):
            t = turn_of * slices + s
            query_weights(t).wait()
            for held, h in enumerate(hops):
                acc[held] += dot(buf[h - 1, s] if h else own(s)[...], wb[lax.rem(t, 2), lax.rem(t, 3)])

            @pl.when(t + 6 < (last + 1) * slices)
            def _():
                query_weights(t + 6).start()

        lax.fori_loop(0, slices, one, None)
        for held, h in enumerate(hops):
            turn(h, ((0, held),))

    def step(i, _):
        @pl.when(i == 1)
        def _():
            late()
            for t in range(6):
                query_weights(t).start()

        @pl.when(i == 2)
        def _():
            queries((2,), 0, 1)

        @pl.when(i == 3)
        def _():
            queries((*range(3, n), 0), 1, 1)
            sent(0)
            for s in range(slices):
                x_slice(s).start()

        @pl.when(i > 1)
        def _():
            attend(i)

        @pl.when(i == n)
        def _():
            for k in range(2, 2 * n - 3):
                sent(k)

        k = n - 2 + i
        mine = k - 1 - (n - 2) * lax.div(1, i)

        def ship(c):
            @pl.when(i < n)
            def _():
                for way in range(2):
                    hop(way, k, c, mine).start()

        def chunk(c, _):
            t = (i - 1) * slices + c
            out_weights(t).wait()
            term[...] = dot(ob[...], wob[lax.rem(t, wos)])

            @pl.when(t + wos < total)
            def _():
                out_weights(t + wos).start()

            @pl.when(c > 0)
            def _():
                ship(c - 1)

            @pl.when(i > 1)
            def _():
                arrive(k - 1, c)
                term[...] += buf[k - 1, c].astype(jnp.float32)

            @pl.when(i < n)
            def _():
                buf[mine, c] = term[...].astype(buf.dtype)

            @pl.when(i == n)
            def _():
                x_slice(c).wait()
                own(c)[...] = (own(c)[...].astype(jnp.float32) + term[...]).astype(y_ref.dtype)
                for way in range(2):
                    hop(way, 2 * n - 3, c).wait_send()

        lax.fori_loop(0, slices, chunk, None)

        ship(slices - 1)

    lax.fori_loop(1, n + 1, step, None)


def tables(tokens):
    half = HEAD // 2
    power = np.power(np.float32(THETA), -np.arange(half, dtype=np.float32) / np.float32(half)).astype(np.float32)
    angle = np.arange(tokens, dtype=np.float32)[:, None] * power
    return np.concatenate([np.cos(angle), np.sin(angle)], 1).astype(np.float32)


def solution(mesh):
    n = mesh.shape["tp"]

    def step(x, gain, wq, wk, wv, wo):
        rows, depth = x.shape
        columns = wq.shape[1]
        heads = columns // HEAD
        slices = depth // SLICE
        tokens = n * rows
        bf16, f32 = jnp.bfloat16, jnp.float32
        whole = pl.BlockSpec(memory_space=pltpu.VMEM)
        hbm = pl.BlockSpec(memory_space=pl.ANY)
        return pl.pallas_call(
            functools.partial(kernel, n, heads // 2),
            out_shape=pltpu.VMEM((rows, depth), bf16),
            in_specs=[hbm, hbm, hbm, hbm, hbm, hbm, hbm],
            out_specs=whole,
            scratch_shapes=[
                pltpu.VMEM((depth,), bf16),
                pltpu.VMEM((tokens, HEAD), f32),
                pltpu.VMEM((2 * n - 2, slices, rows, SLICE), bf16),
                pltpu.VMEM((2, 3, SLICE, columns), bf16),
                pltpu.VMEM((3, rows, columns), f32),
                pltpu.VMEM((tokens, columns), bf16),
                pltpu.VMEM((tokens, columns), bf16),
                pltpu.VMEM((heads, AUG, tokens), bf16),
                pltpu.VMEM((2, columns, SLICE), bf16),
                pltpu.VMEM((rows, columns), bf16),
                pltpu.VMEM((rows, SLICE), f32),
                pltpu.VMEM((2, heads, 1, rows // 2), f32),
                pltpu.VMEM((2, heads, AUG, rows // 2), f32),
                pltpu.SemaphoreType.DMA((2, 2 * n - 2, slices)),
                pltpu.SemaphoreType.DMA((2, 2 * n - 2, slices)),
                pltpu.SemaphoreType.DMA((2, 3)),
                pltpu.SemaphoreType.DMA((2,)),
                pltpu.SemaphoreType.DMA((slices,)),
                pltpu.SemaphoreType.DMA((2,)),
            ],
            compiler_params=pltpu.CompilerParams(collective_id=0, has_side_effects=True, vmem_limit_bytes=63_300_000),
        )(x, gain, tables(tokens), wq, wk, wv, wo)

    tokens, columns = P(("dp", "tp"), None), P(None, "tp")
    return jax.shard_map(
        step,
        mesh=mesh,
        in_specs=(tokens, P(None), columns, columns, columns, P("tp", None)),
        out_specs=tokens,
        check_vma=False,
    )
```
